256 devices in a mesh: groups: 4 (over x, y), tp: 32 (over z), role: 2 (over core).
Axes of the slice: x: 2, y: 2, z: 32, core: 2. Of those that a mesh axis runs over, the one named last changes fastest.
The devices are a block of a 4x8x32 slice.
Arguments:
- rows_in: bfloat16 [2, 2048, 8192], P('role', 'groups', 'tp'), parts along dimension 1, may hold values from -6 to 6
- norm_gain: bfloat16 [8192], replicated, may hold values from 0.5 to 4
- q_words: int32 [1024, 8192], P(None, 'tp'), may hold values from -2147483648 to 2147483646
- q_scales: bfloat16 [64, 8192], P(None, 'tp'), may hold values from 0.0011978149 to 0.0047912598
- kv_words: int32 [32, 1024, 256], P('tp'), may hold values from -2147483648 to 2147483646, as said below
- kv_scales: bfloat16 [32, 64, 256], P('tp'), may hold values from 0.0012 to 0.0048, as said below
- o_words: int32 [1024, 8192], P('tp'), may hold values from -2147483648 to 2147483646
- o_scales: bfloat16 [64, 8192], P('tp'), may hold values from 0.0011978149 to 0.0047912598
- kv_pool: bfloat16 [32, 4096, 16, 256], P('tp', 'groups'), parts along dimension 1, may hold values from -120 to 120, as said below
- prompt_pages: int32 [64], P('groups'), parts along dimension 0, may hold values from 1 to 8, 32 in all
- page_slots: int32 [128], P('groups'), parts along dimension 0, may hold values from 0 to 1023, as said below
- block_tables: int32 [1984, 16], P('groups'), parts along dimension 0, may hold values from 0 to 1023, as said below
- cache_lens: int32 [1984], P('groups'), parts along dimension 0, may hold values from 1 to 256
Outputs:
- layer_out: bfloat16 [2, 2048, 8192], P('role', 'groups', 'tp'), parts along dimension 1
The draws below stay inside these ranges and needn't reach their ends.
There are 4 independent parts, one for each index of `groups`. The reference program is written for one: setup_inputs(seed, part) draws one part's arguments, and reference() takes and returns one part's arrays. A program takes and returns all parts, laid end to end along the dimension named above; an argument that names none is the same for every part. Nothing has to cross between parts.
Inputs may be any that keep to these rules, and one draw needn't show every extreme that they name: `kv_words`: entries t and u are equal whenever t * 8 // 32 equals u * 8 // 32. `kv_scales`: entries t and u are equal whenever t * 8 // 32 equals u * 8 // 32. `kv_pool`: entries t and u are equal whenever t * 8 // 32 equals u * 8 // 32. `page_slots`: distinct pages; entry j receives the j-th page of the prompts taken in order. `block_tables`: no entry is one of page_slots; sequences may share pages.
All inputs are finite; a program needn't handle non-finite values.
Results may differ from the reference program's by a relative error of at most 0.015.
The reference program's roundings to bfloat16 on the way count: a program that leaves them out, or rounds other values in their place, can miss the bound.
Values may be sent and summed in bfloat16 or wider, within the bound.
A program may use at most 192 MiB of HBM per device.

```python
import math
import jax
import jax.numpy as jnp
import numpy as np
from jax import lax

D = 8192
QH = 64
KVH = 8
HD = 128
GROUP = 128
PAGE = 16
PROMPTS = 16
MAXP = 16
ROWS = 512
POOL = 1024
MOSTP = 8
N_TP = 32


def slot_tables(key):
    fresh_count = ROWS // PAGE
    order = jax.random.permutation(jax.random.fold_in(key, 11), POOL).astype(jnp.int32)
    fresh = order[:fresh_count]
    spare = order[fresh_count:]
    picks = jax.random.randint(jax.random.fold_in(key, 12), (ROWS - PROMPTS, MAXP), 0, POOL - fresh_count, dtype=jnp.int32)
    return (fresh, spare[picks])


def draw_page_slots(key, part):
    return slot_tables(key)[0]


def draw_block_tables(key, part):
    return slot_tables(key)[1]


def head_copies(values):
    return jnp.repeat(values, N_TP // KVH, axis=0)


def draw_kv_words(key, part):
    words = jax.random.randint(jax.random.fold_in(key, 21), (KVH, D // 8, 2 * HD), -2147483648, 2147483647, dtype=jnp.int32)
    return head_copies(words)


def draw_kv_scales(key, part):
    logs = jax.random.uniform(jax.random.fold_in(key, 22), (KVH, D // GROUP, 2 * HD), jnp.float32, math.log(0.00121), math.log(0.00476))
    return head_copies(jnp.exp(logs)).astype(jnp.bfloat16)


def draw_kv_pool(key, part):
    values = jnp.clip(jax.random.normal(jax.random.fold_in(key, 23), (KVH, POOL, PAGE, 2 * HD), jnp.float32), -6.0, 6.0)
    return head_copies(values).astype(jnp.bfloat16)


def draw_norm_gain(key, part):
    gains = 1.0 + 0.1 * jnp.clip(jax.random.normal(jax.random.fold_in(key, 24), (D,), jnp.float32), -4.0, 4.0)
    return gains.astype(jnp.bfloat16)


def set_ends(result, rng, least, top_value):
    dims = result.shape
    index_at = [jax.random.randint(jax.random.fold_in(rng, axis), (), 0, dims[axis]) for axis in range(len(dims))]
    result = result.at[tuple(index_at)].set(least)
    longest = dims.index(max(dims))
    index_at[longest] = (index_at[longest] + 1) % dims[longest]
    return result.at[tuple(index_at)].set(top_value)


def steps_of(key, shape, pieces, least, largest):
    level, own = 1.0, jax.random.fold_in(key, 6)
    for position, blocks in pieces:
        heights = jnp.exp(jax.random.uniform(jax.random.fold_in(own, position), (blocks,), jnp.float32, least / len(pieces), largest / len(pieces)))
        level = level * jnp.repeat(heights, shape[position] // blocks).reshape([-1 if axis == position else 1 for axis in range(len(shape))])
    return level


def split_up(number_of, total, bound, lean):
    weights = [(1 << 20) // math.isqrt(standing ** lean) + 1 for standing in range(2, number_of + 1)]
    rest, holding = total - bound - (number_of - 1), [1] * (number_of - 1)
    while rest > 0:
        free = [i for i in range(number_of - 1) if holding[i] < bound]
        mass, remaining = sum([weights[i] for i in free]), rest
        for i in free:
            more = min(bound - holding[i], max(1, remaining * weights[i] // mass), rest)
            holding[i] = holding[i] + more
            rest = rest - more
    return np.array([bound] + holding)


def uneven(stream_key, amount, total, bound, lean):
    if amount == 2:
        one = jax.random.randint(stream_key, (), max(1, total - bound), min(bound, total - 1) + 1)
        return jnp.stack([one, total - one])
    sizes = jnp.asarray(split_up(amount, total, bound, lean), jnp.int32)
    couples = (amount - 1) // 2
    donor, taker = sizes[1:1 + 2 * couples:2], sizes[2:2 + 2 * couples:2]
    margin = jnp.minimum(donor - 1, bound - taker)
    shifted = jax.random.randint(jax.random.fold_in(stream_key, 1), (couples,), 0, 1 << 20) % (margin + 1)
    sizes = sizes.at[1:1 + 2 * couples:2].set(donor - shifted).at[2:2 + 2 * couples:2].set(taker + shifted)
    return sizes[jax.random.permutation(jax.random.fold_in(stream_key, 2), amount)]


def centred(stream_key, extent, scale, reach, pieces=(), kind=jnp.bfloat16):
    array = scale * jax.random.normal(stream_key, extent, jnp.float32)
    if pieces:
        array = array * steps_of(stream_key, extent, pieces, -0.22, 0.18)
    return jnp.clip(array, -reach, reach).astype(kind)


def setup_inputs(seed: int = 0, part: int = 0) -> dict:
    streams_of = jax.random.split(jax.random.key(seed), 14)
    part_splits = jax.random.split(jax.random.fold_in(streams_of[13], part), 14)
    rows_in = centred(part_splits[0], (2, ROWS, D), 1.0, 6.0, ((0, 2), (2, 32)))
    norm_gain = draw_norm_gain(jax.random.fold_in(streams_of[13], 71), part)
    q_words = set_ends(jax.random.randint(streams_of[2], (D // 8, QH * HD), -2147483648, 2147483647), jax.random.fold_in(streams_of[2], 1), -2147483648, 2147483646).astype(jnp.int32)
    q_scales = jnp.clip(jnp.exp(math.log(0.0047912598) - 1.3862944 * jax.random.uniform(streams_of[3], (D // GROUP, QH * HD), jnp.float32) ** steps_of(streams_of[3], (D // GROUP, QH * HD), ((1, 32),), -0.2, 0.2)), 0.0011978149, 0.0047912598).astype(jnp.bfloat16)
    kv_words = draw_kv_words(jax.random.fold_in(streams_of[13], 71), part)
    kv_scales = draw_kv_scales(jax.random.fold_in(streams_of[13], 71), part)
    o_words = set_ends(jax.random.randint(streams_of[6], (QH * HD // 8, D), -2147483648, 2147483647), jax.random.fold_in(streams_of[6], 1), -2147483648, 2147483646).astype(jnp.int32)
    o_scales = jnp.clip(jnp.exp(math.log(0.0047912598) - 1.3862944 * jax.random.uniform(streams_of[7], (QH * HD // GROUP, D), jnp.float32) ** steps_of(streams_of[7], (QH * HD // GROUP, D), ((0, 32),), -0.2, 0.2)), 0.0011978149, 0.0047912598).astype(jnp.bfloat16)
    kv_pool = draw_kv_pool(jax.random.fold_in(jax.random.fold_in(streams_of[13], part), 71), part)
    prompt_pages = uneven(part_splits[9], PROMPTS, ROWS // PAGE, MOSTP, 2).astype(jnp.int32)
    page_slots = draw_page_slots(jax.random.fold_in(jax.random.fold_in(streams_of[13], part), 71), part)
    block_tables = draw_block_tables(jax.random.fold_in(jax.random.fold_in(streams_of[13], part), 71), part)
    cache_lens = set_ends(jax.random.randint(part_splits[12], (ROWS - PROMPTS,), 1, MAXP * PAGE + 1), jax.random.fold_in(part_splits[12], 1), 1, MAXP * PAGE).astype(jnp.int32)
    return dict(rows_in=rows_in, norm_gain=norm_gain, q_words=q_words, q_scales=q_scales, kv_words=kv_words, kv_scales=kv_scales, o_words=o_words, o_scales=o_scales, kv_pool=kv_pool, prompt_pages=prompt_pages, page_slots=page_slots, block_tables=block_tables, cache_lens=cache_lens)


def unpack_words(words, scales):
    shifts = jnp.arange(8, dtype=jnp.int32) * 4
    nibbles = jnp.bitwise_and(jnp.right_shift(words[:, None, :], shifts[None, :, None]), 15) - 8
    values = nibbles.reshape(words.shape[0] * 8, words.shape[1]).astype(jnp.float32)
    group = values.shape[0] // scales.shape[0]
    spread = jnp.repeat(scales.astype(jnp.float32), group, axis=0)
    return (values * spread).astype(jnp.bfloat16)

def rms_normed(rows, gain):
    wide = rows.astype(jnp.float32)
    inverse = lax.rsqrt(lax.optimization_barrier(jnp.mean(wide * wide, axis=-1, keepdims=True)) + 1e-05)
    return (wide * inverse * gain.astype(jnp.float32)).astype(jnp.bfloat16)

def rotate(heads, positions):
    half = heads.shape[-1] // 2
    freq = 500000.0 ** (-jnp.arange(half, dtype=jnp.float32) * 2.0 / heads.shape[-1])
    angle = positions.astype(jnp.float32)[:, None, None] * freq[None, None, :]
    cosine = jnp.cos(angle)
    sine = jnp.sin(angle)
    first = heads[..., :half]
    second = heads[..., half:]
    return jnp.concatenate([first * cosine - second * sine, second * cosine + first * sine], axis=-1)

def layout(prompt_pages, page_slots, block_tables, cache_lens, rows):
    page = rows // page_slots.shape[0]
    count = prompt_pages.shape[0]
    ends = (jnp.cumsum(prompt_pages) * page).astype(jnp.int32)
    starts = (ends - prompt_pages * page).astype(jnp.int32)
    index = jnp.arange(rows, dtype=jnp.int32)
    member = (index[:, None] >= starts[None, :]) & (index[:, None] < ends[None, :])
    doc = lax.optimization_barrier(jnp.sum(jnp.where(member, jnp.arange(count, dtype=jnp.int32)[None, :], 0), axis=1)).astype(jnp.int32)
    prefill_pos = (index - lax.optimization_barrier(jnp.sum(jnp.where(member, starts[None, :], 0), axis=1))).astype(jnp.int32)
    span = block_tables.shape[1]
    picks = jnp.minimum(starts[:, None] // page + jnp.arange(span, dtype=jnp.int32)[None, :], page_slots.shape[0] - 1)
    prompt_table = page_slots[picks.astype(jnp.int32)]
    table = jnp.concatenate([prompt_table, block_tables], axis=0).astype(jnp.int32)
    lengths = jnp.concatenate([prompt_pages * page, cache_lens]).astype(jnp.int32)
    return (doc, prefill_pos, table, lengths)

def prefill_attend(query, keys, values, doc):
    rows = query.shape[0]
    block = min(512, rows)
    score_scale = query.shape[-1] ** (-0.5)
    index = jnp.arange(rows, dtype=jnp.int32)

    def one_block(start):
        partial_query = lax.dynamic_slice_in_dim(query, start, block, 0).astype(jnp.float32)
        logit_scores = jnp.einsum('qhd,kd->hqk', partial_query, keys.astype(jnp.float32)) * score_scale
        own = start + jnp.arange(block, dtype=jnp.int32)
        own_doc = lax.dynamic_slice_in_dim(doc, start, block, 0)
        allowed = (own_doc[:, None] == doc[None, :]) & (index[None, :] <= own[:, None])
        logit_scores = jnp.where(allowed[None], logit_scores, -1e+30)
        attention_probs = jax.nn.softmax(logit_scores, axis=-1).astype(jnp.bfloat16)
        return jnp.einsum('hqk,kd->qhd', attention_probs.astype(jnp.float32), values.astype(jnp.float32)).astype(jnp.bfloat16)
    starts = jnp.arange(0, rows, block, dtype=jnp.int32)
    done = lax.map(one_block, starts)
    return done.reshape(rows, query.shape[1], query.shape[2])

def decode_attend(query, key_self, value_self, cache, table, lengths):
    rows = query.shape[0]
    block = min(128, rows)
    score_scale = query.shape[-1] ** (-0.5)
    head_dim = query.shape[-1]

    def one_block(start):
        partial_query = lax.dynamic_slice_in_dim(query, start, block, 0).astype(jnp.float32)
        part_table = lax.dynamic_slice_in_dim(table, start, block, 0)
        part_len = lax.dynamic_slice_in_dim(lengths, start, block, 0)
        pages = cache[part_table]
        pages = pages.reshape(block, pages.shape[1] * pages.shape[2], pages.shape[3])
        own_key = lax.dynamic_slice_in_dim(key_self, start, block, 0)
        own_value = lax.dynamic_slice_in_dim(value_self, start, block, 0)
        gathered_keys = jnp.concatenate([pages[..., :head_dim], own_key[:, None, :]], axis=1)
        gathered_values = jnp.concatenate([pages[..., head_dim:], own_value[:, None, :]], axis=1)
        logit_scores = jnp.einsum('jai,jri->jar', partial_query, gathered_keys.astype(jnp.float32)) * score_scale
        spots = jnp.arange(pages.shape[1], dtype=jnp.int32)
        valid = jnp.concatenate([spots[None, :] < part_len[:, None], jnp.ones((block, 1), dtype=bool)], axis=1)
        logit_scores = jnp.where(valid[:, None, :], logit_scores, -1e+30)
        attention_probs = jax.nn.softmax(logit_scores, axis=-1).astype(jnp.bfloat16)
        return jnp.einsum('cwt,ctr->cwr', attention_probs.astype(jnp.float32), gathered_values.astype(jnp.float32)).astype(jnp.bfloat16)
    starts = jnp.arange(0, rows, block, dtype=jnp.int32)
    done = lax.map(one_block, starts)
    return done.reshape(rows, query.shape[1], query.shape[2])

def reference(rows_in, norm_gain, q_words, q_scales, kv_words, kv_scales, o_words, o_scales, kv_pool, prompt_pages, page_slots, block_tables, cache_lens):
    copies = N_TP // KVH
    group_heads = QH // KVH
    doc, prefill_pos, table, lengths = layout(prompt_pages, page_slots, block_tables, cache_lens, ROWS)
    w_query = unpack_words(q_words, q_scales)
    w_out = unpack_words(o_words, o_scales)
    normed = [rms_normed(rows_in[0], norm_gain), rms_normed(rows_in[1], norm_gain)]
    positions = [prefill_pos, lengths]
    queries = []
    for side in range(2):
        projected = jnp.dot(normed[side], w_query, preferred_element_type=jnp.float32).reshape(ROWS, QH, HD)
        queries.append(rotate(projected, positions[side]).astype(jnp.bfloat16))
    attention_output = [[], []]
    for head in range(KVH):
        w_keyval = unpack_words(kv_words[head * copies], kv_scales[head * copies])
        keys = []
        values = []
        for side in range(2):
            keyval = jnp.dot(normed[side], w_keyval, preferred_element_type=jnp.float32)
            keys.append(rotate(keyval[:, None, :HD], positions[side])[:, 0].astype(jnp.bfloat16))
            values.append(keyval[:, HD:].astype(jnp.bfloat16))
        fresh = jnp.concatenate([keys[0], values[0]], axis=1).reshape(ROWS // PAGE, PAGE, 2 * HD)
        cache = kv_pool[head * copies].at[page_slots].set(fresh)
        lower = head * group_heads
        attention_output[0].append(prefill_attend(queries[0][:, lower:lower + group_heads], keys[0], values[0], doc))
        attention_output[1].append(decode_attend(queries[1][:, lower:lower + group_heads], keys[1], values[1], cache, table, lengths))
    results = []
    for side in range(2):
        joined = jnp.concatenate(attention_output[side], axis=1).reshape(ROWS, QH * HD)
        results.append(jnp.dot(joined, w_out, preferred_element_type=jnp.float32).astype(jnp.bfloat16))
    return jnp.stack(results)
```

```python
import functools

import jax
import jax.numpy as jnp
from jax import lax
from jax.experimental import pallas as pl
from jax.experimental.pallas import tpu as pltpu
from jax.sharding import PartitionSpec as P

HD = 128
LONGEST = 128
MESH = pl.DeviceIdType.MESH
VMEM = pltpu.VMEM


def nibble_order(width):
    words = width // 8
    source = lax.broadcasted_iota(jnp.int32, (width, width), 0)
    column = lax.broadcasted_iota(jnp.int32, (width, width), 1)
    wanted = lax.rem(column, words) * 8 + column // words
    return jnp.where(source == wanted, 1.0, 0.0).astype(jnp.bfloat16)


def unpack_into(target, lane, words, low_scale, high_scale):
    count, width = words.shape
    half = count // 2
    scale = jnp.concatenate(
        [
            jnp.broadcast_to(low_scale, (half, width)),
            jnp.broadcast_to(high_scale, (half, width)),
        ],
        axis=0,
    )
    for k in range(8):
        nibble = jnp.bitwise_and(jnp.right_shift(words, 4 * k), 15) - 8
        value = (nibble.astype(jnp.float32) * scale).astype(jnp.bfloat16)
        target[k * count : (k + 1) * count, lane : lane + width] = value


def ring(n):
    me = lax.axis_index("tp")
    return me, lax.rem(me + 1, n), lax.rem(me + n - 1, n)


def signal_ready(peers):
    barrier = pltpu.get_barrier_semaphore()
    for peer in peers:
        pl.semaphore_signal(barrier, inc=1, device_id=peer, device_id_type=MESH)
    return barrier


def gather_project(
    n, x_ref, q_words, kv_words, q_scales, kv_scales, gain_ref, cos_ref, sin_ref,
    q_out, kv_out, fresh_out,
    xbuf, stat, acc, weights, inverse, gains, scales, qw, kw, arrived,
    load_sem, recv_right, recv_left, stat_right, stat_left, send_sem, stat_send, pair_sem,
):
    me, right, left = ring(n)
    role = lax.axis_index("role")
    half, turn = n // 2, n // 4
    rows, width = x_ref.shape
    sub = rows // 4

    barrier = signal_ready(({"tp": right}, {"tp": left}, {"role": 1 - role}))
    loads = (
        pltpu.make_async_copy(q_words, qw, load_sem.at[0]),
        pltpu.make_async_copy(kv_words, kw, load_sem.at[1]),
    )
    for load in loads:
        load.start()

    order = nibble_order(width)
    x = x_ref[...]
    xbuf[me] = jnp.dot(x, order, preferred_element_type=jnp.float32).astype(jnp.bfloat16)
    wide = x.astype(jnp.float32)
    squares = wide * wide
    folded = squares[:, 0:128]
    for lane in range(128, width, 128):
        folded = folded + squares[:, lane : lane + 128]
    stat[me] = jnp.sum(folded.T, axis=0, keepdims=True)
    gains[...] = jnp.dot(gain_ref[...], order, preferred_element_type=jnp.float32)
    scales[:, 0:width] = q_scales[...].astype(jnp.float32)
    scales[:, width:] = kv_scales[...].astype(jnp.float32)
    acc[...] = jnp.zeros_like(acc)

    def data(chunk, hop, u, to_right):
        piece = xbuf.at[chunk, pl.ds(u * sub, sub), :]
        return pltpu.make_async_remote_copy(
            src_ref=piece,
            dst_ref=piece,
            send_sem=send_sem,
            recv_sem=(recv_right if to_right else recv_left).at[hop, u],
            device_id={"tp": right if to_right else left},
            device_id_type=MESH,
        )

    def figure(chunk, hop, to_right):
        return pltpu.make_async_remote_copy(
            src_ref=stat.at[chunk],
            dst_ref=stat.at[chunk],
            send_sem=stat_send,
            recv_sem=(stat_right if to_right else stat_left).at[hop],
            device_id={"tp": right if to_right else left},
            device_id_type=MESH,
        )

    def behind(s):
        return lax.rem(me + n - s, n)

    def ahead(s):
        return lax.rem(me + s, n)

    def pass_figures(h):
        figure(behind(h), h - 1, True).wait_recv()
        figure(behind(h), h, True).start()
        figure(ahead(h), h - 1, False).wait_recv()
        figure(ahead(h), h, False).start()

    def pass_data(s, u):
        data(behind(s), s - 1, u, True).wait_recv()
        data(behind(s), s, u, True).start()
        data(ahead(s), s - 1, u, False).wait_recv()
        data(ahead(s), s, u, False).start()

    def project(chunk):
        low = scales[pl.ds(2 * chunk, 1), :]
        high = scales[pl.ds(2 * chunk + 1, 1), :]
        first = pl.multiple_of(chunk * (width // 8), width // 8)
        for lane, words in ((0, qw), (width, kw)):
            unpack_into(
                weights, lane, words[pl.ds(first, width // 8), :],
                low[:, lane : lane + width], high[:, lane : lane + width],
            )
        gain = gains[pl.ds(chunk, 1), :]
        for u in range(4):
            part = pl.ds(u * sub, sub)
            scale = inverse[part, :]
            scale = jnp.concatenate([scale] * (width // 128), axis=1)
            normed = (xbuf[chunk, part, :].astype(jnp.float32) * scale * gain).astype(jnp.bfloat16)
            acc[part, :] += jnp.dot(normed, weights[...], preferred_element_type=jnp.float32)

    pl.semaphore_wait(barrier, 3)
    figure(me, 0, True).start()
    figure(me, 0, False).start()
    for u in range(4):
        data(me, 0, u, True).start()
        data(me, 0, u, False).start()
    for load in loads:
        load.wait()
    pass_figures(1)

    @pl.loop(1, turn)
    def _(s):
        for u in range(4):
            pass_data(s, u)
            if u == 1:
                pass_figures(2 * s)
            if u == 3:

                @pl.when(2 * s + 1 < half - 1)
                def _():
                    pass_figures(2 * s + 1)

                @pl.when(2 * s + 1 == half - 1)
                def _():
                    figure(behind(half - 1), half - 2, True).wait_recv()
                    figure(behind(half - 1), half - 1, True).start()
                    figure(ahead(half - 1), half - 2, False).wait_recv()

    figure(behind(half), half - 1, True).wait_recv()
    total = stat[0]
    for i in range(1, n):
        total = total + stat[i]
    mean = total / (n * width)
    inverse[...] = jnp.broadcast_to(lax.rsqrt(mean + 1e-05), (128, rows)).T

    @pl.loop(turn, half - 1)
    def _(s):
        for u in range(4):
            pass_data(s, u)
            o = 4 * (s - turn) + u
            project(behind((o + 1) // 2) if u % 2 else ahead(o // 2))

    last = half - 1
    for u in range(4):
        data(behind(last), last - 1, u, True).wait_recv()
        if u < 2:
            data(behind(last), last, u, True).start()
        data(ahead(last), last - 1, u, False).wait_recv()
        if u >= 2:
            data(ahead(last), last, u, False).start()
    project(ahead(last - 1))
    project(behind(last))
    project(ahead(last))
    for u in range(4):
        data(behind(half), last, u, u < 2).wait_recv()
    project(behind(half))

    cosine, sine = cos_ref[...], sin_ref[...]

    def rotated(lane):
        head = acc[:, lane : lane + HD]
        return (head * cosine + pltpu.roll(head, HD // 2, 1) * sine).astype(jnp.bfloat16)

    kv_out[:, 0:HD] = rotated(width)
    kv_out[:, HD:] = acc[:, width + HD :].astype(jnp.bfloat16)
    for lane in range(0, width, HD):
        q_out[:, lane : lane + HD] = rotated(lane)
    swap = pltpu.make_async_remote_copy(
        src_ref=kv_out, dst_ref=arrived, send_sem=pair_sem.at[0], recv_sem=pair_sem.at[1],
        device_id={"role": 1 - role}, device_id_type=MESH,
    )

    @pl.when(role == 0)
    def _():
        swap.start()
        fresh_out[...] = kv_out[...]
        swap.wait_send()

    @pl.when(role == 1)
    def _():
        swap.wait_recv()
        fresh_out[...] = arrived[...]

    every = xbuf.at[pl.ds(0, n - 1)]
    pltpu.make_async_copy(every, every, send_sem).wait()
    every = stat.at[pl.ds(0, n - 1)]
    pltpu.make_async_copy(every, every, stat_send).wait()


def project_scatter(
    n, att_ref, o_words, scale_ref, out_ref,
    attended, ow, weights, part, begun, slots, load_sem, recv_right, recv_left, send_sem,
):
    me, right, left = ring(n)
    half = n // 2
    rows, width = att_ref.shape
    sub = rows // 4
    barrier = signal_ready(({"tp": right}, {"tp": left}))
    load = pltpu.make_async_copy(o_words, ow, load_sem)
    load.start()
    attended[...] = jnp.dot(
        att_ref[...], nibble_order(width), preferred_element_type=jnp.float32
    ).astype(jnp.bfloat16)
    load.wait()

    def unpack(side, dest):
        columns = pl.ds(pl.multiple_of(dest * width, width), width)
        scale = scale_ref[:, columns].astype(jnp.float32)
        unpack_into(weights.at[side], 0, ow[:, columns], scale[0:1, :], scale[1:2, :])

    def multiply(side, u):
        piece = pl.ds(u * sub, sub)
        part[side, piece, :] = jnp.dot(
            attended[piece, :], weights[side], preferred_element_type=jnp.float32
        )

    def dest(side, s):
        return lax.rem(me + half + (s if side else n - s), n)

    def token(source, side, hop, u):
        piece = pl.ds(u * sub, sub)
        return pltpu.make_async_remote_copy(
            src_ref=source.at[piece, :],
            dst_ref=slots.at[side * half + hop, piece, :],
            send_sem=send_sem,
            recv_sem=(recv_left if side else recv_right).at[hop, u],
            device_id={"tp": left if side else right},
            device_id_type=MESH,
        )

    def slot(side, hop):
        return slots.at[side * half + hop]

    unpack(0, dest(0, 0))
    for u in range(4):
        multiply(0, u)
    begun[...] = part[0].astype(jnp.bfloat16)
    pl.semaphore_wait(barrier, 2)
    for u in range(4):
        token(begun, u // 2, 0, u).start()
    for side in range(2):
        unpack(side, dest(side, 1))
        for u in range(4):
            multiply(side, u)

    def step(s, joins):
        for side in range(2):
            unpack(side, dest(side, s + 1))
        for u in range(4):
            piece = pl.ds(u * sub, sub)
            for side in range(2):
                here = slot(side, s - 1)
                term = part[side, piece, :]
                if joins(side, u):
                    token(here, side, s - 1, u).wait_recv()
                    term = term + here[piece, :].astype(jnp.float32)
                here[piece, :] = term.astype(jnp.bfloat16)
                multiply(side, u)
                token(here, side, s, u).start()

    step(1, lambda side, u: side == u // 2)

    @pl.loop(2, half)
    def _(s):
        step(s, lambda side, u: True)

    for u in range(4):
        piece = pl.ds(u * sub, sub)
        term = part[0, piece, :]
        for side in range(2):
            here = slot(side, half - 1)
            token(here, side, half - 1, u).wait_recv()
            term = term + here[piece, :].astype(jnp.float32)
        out_ref[piece, :] = term.astype(jnp.bfloat16)
    every = slots.at[pl.ds(0, n - 1)]
    pltpu.make_async_copy(every, every, send_sem).wait()


def prefill_kernel(start_ref, q_ref, kv_ref, out_ref):
    rows = q_ref.shape[0]
    block = min(LONGEST, rows)
    for first in range(0, rows, block):
        low = max(0, first - LONGEST)
        count = first + block - low
        keys = kv_ref[low : first + block, 0:HD]
        values = kv_ref[low : first + block, HD:]
        row = lax.broadcasted_iota(jnp.int32, (block, count), 0) + first
        key = lax.broadcasted_iota(jnp.int32, (block, count), 1) + low
        allowed = (key <= row) & (key >= start_ref[first : first + block, :])
        for lane in range(0, q_ref.shape[1], HD):
            query = q_ref[first : first + block, lane : lane + HD]
            scores = lax.dot_general(
                query, keys, (((1,), (1,)), ((), ())), preferred_element_type=jnp.float32
            ) * (HD**-0.5)
            scores = jnp.where(allowed, scores, -1e30)
            top = jnp.max(scores, axis=1, keepdims=True)
            raised = jnp.exp(scores - top)
            weight = raised * (1.0 / jnp.sum(raised, axis=1, keepdims=True))
            out_ref[first : first + block, lane : lane + HD] = jnp.dot(
                weight.astype(jnp.bfloat16), values, preferred_element_type=jnp.float32
            ).astype(jnp.bfloat16)


def decode_kernel(
    table_ref, length_ref, q_ref, kv_ref, fresh_ref, pool_ref, out_ref,
    cache, q_wide, kv_wide, out_wide, load_sem,
):
    rows = q_ref.shape[0]
    pool, page, _ = pool_ref.shape
    span = table_ref.shape[0] // rows
    load = pltpu.make_async_copy(pool_ref, cache.at[pl.ds(0, pool)], load_sem)
    load.start()
    for j in range(rows // page):
        cache[pool + j] = fresh_ref[j * page : (j + 1) * page, :]
    q_wide[...] = q_ref[...].astype(jnp.float32)
    kv_wide[...] = kv_ref[...].astype(jnp.float32)
    load.wait()
    batch = 8
    owner = lax.rem(lax.broadcasted_iota(jnp.int32, (2 * batch, HD), 0), batch)
    spot = lax.broadcasted_iota(jnp.int32, (2 * batch, span * page), 1)

    def gathered(first, lane):
        pages = []
        for j in range(span):
            pair = [
                cache[table_ref[(first + t) * span + j], :, lane : lane + HD] for t in range(2)
            ]
            pages.append(jnp.concatenate(pair, axis=1))
        return jnp.concatenate(pages, axis=0)

    def one_block(b):
        first = pl.multiple_of(b * batch, batch)
        piece = pl.ds(first, batch)
        both = q_wide[piece, :]
        query = jnp.concatenate([both[:, 0:HD], both[:, HD:]], axis=0)
        own = kv_wide[piece, :]
        own_key = jnp.concatenate([own[:, 0:HD]] * 2, axis=0)
        own_value = jnp.concatenate([own[:, HD:]] * 2, axis=0)
        length = length_ref[piece, :]
        length = jnp.concatenate([length] * 2, axis=0)
        scores = None
        for p in range(0, batch, 2):
            mine = jnp.concatenate(
                [jnp.where(owner == p + t, query, 0.0) for t in range(2)], axis=1
            ).astype(jnp.bfloat16)
            term = lax.dot_general(
                mine, gathered(first + p, 0), (((1,), (1,)), ((), ())),
                preferred_element_type=jnp.float32,
            )
            scores = term if scores is None else scores + term
        scores = jnp.where(spot < length, scores * (HD**-0.5), -1e30)
        self_score = jnp.sum(query * own_key, axis=1, keepdims=True) * (HD**-0.5)
        top = jnp.maximum(jnp.max(scores, axis=1, keepdims=True), self_score)
        raised = jnp.exp(scores - top)
        self_raised = jnp.exp(self_score - top)
        share = 1.0 / (jnp.sum(raised, axis=1, keepdims=True) + self_raised)
        weight = (raised * share).astype(jnp.bfloat16)
        total = (self_raised * share).astype(jnp.bfloat16).astype(jnp.float32) * own_value
        for p in range(0, batch, 2):
            term = jnp.dot(weight, gathered(first + p, HD), preferred_element_type=jnp.float32)
            for t in range(2):
                total = total + jnp.where(owner == p + t, term[:, t * HD : (t + 1) * HD], 0.0)
        out_wide[piece, 0:HD] = total[0:batch, :]
        out_wide[piece, HD:] = total[batch:, :]

    @pl.loop(0, rows // batch, step=2)
    def _(b):
        one_block(b)
        one_block(b + 1)

    out_ref[...] = out_wide[...].astype(jnp.bfloat16)


def local(
    rows_in, norm_gain, q_words, q_scales, kv_words, kv_scales, o_words, o_scales,
    kv_pool, prompt_pages, page_slots, block_tables, cache_lens,
):
    n = lax.axis_size("tp")
    side = lax.axis_index("role")
    x = rows_in[0]
    rows, width = x.shape
    half = n // 2
    pool = kv_pool[0]
    page = pool.shape[1]
    count = prompt_pages.shape[0]
    sub_sems = pltpu.SemaphoreType.DMA((half, 4))
    dma = pltpu.SemaphoreType.DMA
    in_vmem = pl.BlockSpec(memory_space=VMEM)
    anywhere = pl.BlockSpec(memory_space=pl.ANY)
    bf16, f32 = jnp.bfloat16, jnp.float32

    ends = jnp.cumsum(prompt_pages) * page
    starts = ends - prompt_pages * page
    index = jnp.arange(rows, dtype=jnp.int32)
    member = (index[:, None] >= starts[None, :]) & (index[:, None] < ends[None, :])
    doc_start = jnp.sum(jnp.where(member, starts[None, :], 0), axis=1)
    lengths = jnp.concatenate([prompt_pages * page, cache_lens])
    positions = jnp.where(side == 0, index - doc_start, lengths)
    freq = 500000.0 ** (-jnp.arange(HD // 2, dtype=f32) * 2.0 / HD)
    angle = positions.astype(f32)[:, None] * freq[None, :]
    cosine, sine = jnp.cos(angle), jnp.sin(angle)
    cosine = jnp.concatenate([cosine, cosine], axis=1)
    sine = jnp.concatenate([-sine, sine], axis=1)

    half_block = jax.ShapeDtypeStruct((rows, width), bf16)
    query, fresh, arrived = pl.pallas_call(
        functools.partial(gather_project, n),
        out_shape=(half_block, jax.ShapeDtypeStruct((rows, 2 * HD), bf16),
                   jax.ShapeDtypeStruct((rows, 2 * HD), bf16)),
        in_specs=[in_vmem, anywhere, anywhere] + [in_vmem] * 5,
        out_specs=(in_vmem, in_vmem, in_vmem),
        scratch_shapes=[
            VMEM((n, rows, width), bf16),
            VMEM((n, 1, rows), f32),
            VMEM((rows, width + 2 * HD), f32),
            VMEM((width, width + 2 * HD), bf16),
            VMEM((rows, 128), f32),
            VMEM((n, width), f32),
            VMEM((q_scales.shape[0], width + 2 * HD), f32),
            VMEM(q_words.shape, jnp.int32),
            VMEM(kv_words.shape[1:], jnp.int32),
            VMEM((rows, 2 * HD), bf16),
            dma((2,)), sub_sems, sub_sems, dma((half,)), dma((half,)),
            dma, dma, dma((2,)),
        ],
        compiler_params=pltpu.CompilerParams(
            collective_id=0, has_side_effects=True, vmem_limit_bytes=40 << 20
        ),
        cost_estimate=pl.CostEstimate(
            flops=4 * n * rows * width * width, bytes_accessed=4 << 20, transcendentals=0
        ),
        name="gather_project",
    )(
        x, q_words, kv_words[0], q_scales, kv_scales[0],
        norm_gain.reshape(n, width), cosine, sine,
    )

    def run_prefill():
        return pl.pallas_call(
            prefill_kernel,
            out_shape=half_block,
            in_specs=[in_vmem] * 3,
            out_specs=in_vmem,
            name="prefill",
        )(doc_start[:, None], query, fresh)

    def run_decode():
        span = block_tables.shape[1]
        own = pool.shape[0] + jnp.minimum(
            starts[:, None] // page + jnp.arange(span, dtype=jnp.int32)[None, :],
            page_slots.shape[0] - 1,
        )
        table = jnp.concatenate([own, block_tables], axis=0).reshape(-1)
        return pl.pallas_call(
            decode_kernel,
            out_shape=half_block,
            in_specs=[pl.BlockSpec(memory_space=pltpu.SMEM)] + [in_vmem] * 4 + [anywhere],
            out_specs=in_vmem,
            scratch_shapes=[
                VMEM((pool.shape[0] + rows // page, page, 2 * HD), bf16),
                VMEM((rows, width), f32),
                VMEM((rows, 2 * HD), f32),
                VMEM((rows, width), f32),
                dma,
            ],
            compiler_params=pltpu.CompilerParams(vmem_limit_bytes=40 << 20),
            name="decode",
        )(table, lengths[:, None], query, fresh, arrived, pool)

    attended = lax.cond(side == 0, run_prefill, run_decode)

    out = pl.pallas_call(
        functools.partial(project_scatter, n),
        out_shape=half_block,
        in_specs=[in_vmem, anywhere, in_vmem],
        out_specs=in_vmem,
        scratch_shapes=[
            VMEM((rows, width), bf16),
            VMEM(o_words.shape, jnp.int32),
            VMEM((2, width, width), bf16),
            VMEM((2, rows, width), f32),
            VMEM((rows, width), bf16),
            VMEM((n, rows, width), bf16),
            dma, sub_sems, sub_sems, dma,
        ],
        compiler_params=pltpu.CompilerParams(
            collective_id=1, has_side_effects=True, vmem_limit_bytes=40 << 20
        ),
        cost_estimate=pl.CostEstimate(
            flops=2 * n * rows * width * width, bytes_accessed=4 << 20, transcendentals=0
        ),
        name="project_scatter",
    )(attended, o_words, o_scales)
    return out[None]


def solution(mesh):
    return jax.shard_map(
        local,
        mesh=mesh,
        in_specs=(
            P("role", "groups", "tp"),
            P(),
            P(None, "tp"),
            P(None, "tp"),
            P("tp", None, None),
            P("tp", None, None),
            P("tp", None),
            P("tp", None),
            P("tp", "groups", None, None),
            P("groups"),
            P("groups"),
            P("groups", None),
            P("groups"),
        ),
        out_specs=P("role", "groups", "tp"),
        check_vma=False,
    )
```

```python
import functools

import jax
import jax.numpy as jnp
import numpy as np
from jax import lax
from jax.experimental import pallas as pl
from jax.experimental.pallas import tpu as pltpu
from jax.sharding import PartitionSpec as P

HD = 128
LONGEST = 128
GATHER_PIECES = 4
SCATTER_PIECES = 8
GATHER_VMEM = 58 << 20
MESH = pl.DeviceIdType.MESH
VMEM = pltpu.VMEM


def nibble_order(width):
    words = width // 8
    source = lax.broadcasted_iota(jnp.int32, (width, width), 0)
    column = lax.broadcasted_iota(jnp.int32, (width, width), 1)
    wanted = lax.rem(column, words) * 8 + column // words
    return jnp.where(source == wanted, 1.0, 0.0).astype(jnp.bfloat16)


def unpack_into(target, lane, words, low_scale, high_scale):
    count, width = words.shape
    half = count // 2
    scale = jnp.concatenate(
        [
            jnp.broadcast_to(low_scale, (half, width)),
            jnp.broadcast_to(high_scale, (half, width)),
        ],
        axis=0,
    )
    for k in range(8):
        nibble = jnp.bitwise_and(jnp.right_shift(words, 4 * k), 15) - 8
        value = (nibble.astype(jnp.float32) * scale).astype(jnp.bfloat16)
        target[k * count : (k + 1) * count, lane : lane + width] = value


def ring(n):
    me = lax.axis_index("tp")
    return me, lax.rem(me + 1, n), lax.rem(me + n - 1, n)


def signal_ready(peers):
    barrier = pltpu.get_barrier_semaphore()
    for peer in peers:
        pl.semaphore_signal(barrier, inc=1, device_id=peer, device_id_type=MESH)
    return barrier


def prompt_start(pages_ref, page, row):
    start, begin = jnp.zeros_like(row), 0
    for p in range(pages_ref.shape[0]):
        end = begin + pages_ref[p] * page
        start = jnp.where((row >= begin) & (row < end), begin, start)
        begin = end
    return start


def gather_project(
    page, n, pages_ref, x_hbm, q_words, kv_words, q_scales, kv_scales, gain_ref,
    length_ref, freq_ref, q_out, kv_out, fresh_out,
    x_ref, xbuf, stat, acc, weights, inverse, gains, scales, qw, kw, arrived, cosine, sine,
    load_sem, recv_right, recv_left, stat_right, stat_left, send_sem, stat_send, pair_sem,
):
    me, right, left = ring(n)
    role = lax.axis_index("role")
    half, turn = n // 2, n // 4
    rows, width = x_ref.shape
    pieces = recv_right.shape[1]
    sub = rows // pieces

    barrier = signal_ready(({"tp": right}, {"tp": left}, {"role": 1 - role}))
    load_x = pltpu.make_async_copy(x_hbm, x_ref, load_sem.at[0])
    loads = (
        pltpu.make_async_copy(q_words, qw, load_sem.at[1]),
        pltpu.make_async_copy(kv_words, kw, load_sem.at[2]),
    )
    load_x.start()
    for load in loads:
        load.start()

    order = nibble_order(width)
    load_x.wait()
    x = x_ref[...]
    xbuf[me] = jnp.dot(x, order, preferred_element_type=jnp.float32).astype(jnp.bfloat16)
    wide = x.astype(jnp.float32)
    squares = wide * wide
    folded = squares[:, 0:128]
    for lane in range(128, width, 128):
        folded = folded + squares[:, lane : lane + 128]
    stat[me] = jnp.sum(folded.T, axis=0, keepdims=True)

    def data(chunk, hop, u, to_right):
        piece = xbuf.at[chunk, pl.ds(u * sub, sub), :]
        return pltpu.make_async_remote_copy(
            src_ref=piece,
            dst_ref=piece,
            send_sem=send_sem,
            recv_sem=(recv_right if to_right else recv_left).at[hop, u],
            device_id={"tp": right if to_right else left},
            device_id_type=MESH,
        )

    def figure(chunk, hop, to_right):
        return pltpu.make_async_remote_copy(
            src_ref=stat.at[chunk],
            dst_ref=stat.at[chunk],
            send_sem=stat_send,
            recv_sem=(stat_right if to_right else stat_left).at[hop],
            device_id={"tp": right if to_right else left},
            device_id_type=MESH,
        )

    def behind(s):
        return lax.rem(me + n - s, n)

    def ahead(s):
        return lax.rem(me + s, n)

    def pass_figures(h):
        figure(behind(h), h - 1, True).wait_recv()
        figure(behind(h), h, True).start()
        figure(ahead(h), h - 1, False).wait_recv()
        figure(ahead(h), h, False).start()

    def pass_data(s, u):
        data(behind(s), s - 1, u, True).wait_recv()
        data(behind(s), s, u, True).start()
        data(ahead(s), s - 1, u, False).wait_recv()
        data(ahead(s), s, u, False).start()

    def project(chunk):
        low = scales[pl.ds(2 * chunk, 1), :]
        high = scales[pl.ds(2 * chunk + 1, 1), :]
        first = pl.multiple_of(chunk * (width // 8), width // 8)
        for lane, words in ((0, qw), (width, kw)):
            unpack_into(
                weights, lane, words[pl.ds(first, width // 8), :],
                low[:, lane : lane + width], high[:, lane : lane + width],
            )
        gain = gains[pl.ds(chunk, 1), :]
        for u in range(4):
            part = pl.ds(u * (rows // 4), rows // 4)
            scale = inverse[part, :]
            scale = jnp.concatenate([scale] * (width // 128), axis=1)
            normed = (xbuf[chunk, part, :].astype(jnp.float32) * scale * gain).astype(jnp.bfloat16)
            acc[part, :] += jnp.dot(normed, weights[...], preferred_element_type=jnp.float32)

    pl.semaphore_wait(barrier, 3)
    figure(me, 0, True).start()
    figure(me, 0, False).start()
    for u in range(pieces):
        data(me, 0, u, True).start()
        data(me, 0, u, False).start()
    gains[...] = jnp.dot(
        gain_ref[...].astype(jnp.bfloat16), order, preferred_element_type=jnp.float32
    )
    scales[:, 0:width] = q_scales[...].astype(jnp.float32)
    scales[:, width:] = kv_scales[...].astype(jnp.float32)
    acc[...] = jnp.zeros_like(acc)
    row = lax.broadcasted_iota(jnp.int32, (rows, HD), 0)
    placed = (row - prompt_start(pages_ref, page, row)).astype(jnp.float32)
    held = jnp.broadcast_to(length_ref[...].astype(jnp.float32), (HD, rows)).T
    angle = jnp.where(role == 0, placed, held) * freq_ref[...]
    cosine[...] = jnp.cos(angle)
    turned = jnp.sin(angle)
    lane = lax.broadcasted_iota(jnp.int32, (rows, HD), 1)
    sine[...] = jnp.where(lane < HD // 2, -turned, turned)
    for load in loads:
        load.wait()
    pass_figures(1)

    quarter = pieces // 4

    @pl.loop(1, turn)
    def _(s):
        for u in range(pieces):
            pass_data(s, u)
            if u == 2 * quarter - 1:
                pass_figures(2 * s)
            if u == pieces - 1:

                @pl.when(2 * s + 1 < half - 1)
                def _():
                    pass_figures(2 * s + 1)

                @pl.when(2 * s + 1 == half - 1)
                def _():
                    figure(behind(half - 1), half - 2, True).wait_recv()
                    figure(behind(half - 1), half - 1, True).start()
                    figure(ahead(half - 1), half - 2, False).wait_recv()

    figure(behind(half), half - 1, True).wait_recv()
    total = stat[0]
    for i in range(1, n):
        total = total + stat[i]
    mean = total / (n * width)
    inverse[...] = jnp.broadcast_to(lax.rsqrt(mean + 1e-05), (128, rows)).T

    @pl.loop(turn, half - 1)
    def _(s):
        for i in range(4):
            for u in range(i * quarter, (i + 1) * quarter):
                pass_data(s, u)
            o = 4 * (s - turn) + i
            project(behind((o + 1) // 2) if i % 2 else ahead(o // 2))

    last = half - 1
    for u in range(pieces):
        data(behind(last), last - 1, u, True).wait_recv()
        if u < pieces // 2:
            data(behind(last), last, u, True).start()
        data(ahead(last), last - 1, u, False).wait_recv()
        if u >= pieces // 2:
            data(ahead(last), last, u, False).start()
    project(ahead(last - 1))
    project(behind(last))
    project(ahead(last))
    for u in range(pieces):
        data(behind(half), last, u, u < pieces // 2).wait_recv()
    project(behind(half))

    def rotated(lane):
        head = acc[:, lane : lane + HD]
        turned = pltpu.roll(head, HD // 2, 1)
        return (head * cosine[...] + turned * sine[...]).astype(jnp.bfloat16)

    kv_out[:, 0:HD] = rotated(width)
    kv_out[:, HD:] = acc[:, width + HD :].astype(jnp.bfloat16)
    for lane in range(0, width, HD):
        q_out[:, lane : lane + HD] = rotated(lane)
    swap = pltpu.make_async_remote_copy(
        src_ref=kv_out, dst_ref=arrived, send_sem=pair_sem.at[0], recv_sem=pair_sem.at[1],
        device_id={"role": 1 - role}, device_id_type=MESH,
    )

    @pl.when(role == 0)
    def _():
        swap.start()
        fresh_out[...] = kv_out[...]
        swap.wait_send()

    @pl.when(role == 1)
    def _():
        swap.wait_recv()
        fresh_out[...] = arrived[...]

    every = xbuf.at[pl.ds(0, n - 1)]
    pltpu.make_async_copy(every, every, send_sem).wait()
    every = stat.at[pl.ds(0, n - 1)]
    pltpu.make_async_copy(every, every, stat_send).wait()


def project_scatter(
    n, att_ref, o_words, scale_ref, out_ref,
    attended, ow, weights, part, begun, slots, load_sem, recv_right, recv_left, send_sem,
):
    me, right, left = ring(n)
    half = n // 2
    rows, width = att_ref.shape
    pieces = recv_right.shape[1]
    sub = rows // pieces
    barrier = signal_ready(({"tp": right}, {"tp": left}))
    load = pltpu.make_async_copy(o_words, ow, load_sem)
    load.start()
    attended[...] = jnp.dot(
        att_ref[...], nibble_order(width), preferred_element_type=jnp.float32
    ).astype(jnp.bfloat16)
    load.wait()

    def unpack(side, dest):
        columns = pl.ds(pl.multiple_of(dest * width, width), width)
        scale = scale_ref[:, columns].astype(jnp.float32)
        unpack_into(weights.at[side], 0, ow[:, columns], scale[0:1, :], scale[1:2, :])

    def multiply(side, turn, i):
        block = pl.ds(i * (rows // 2), rows // 2)
        part[turn, side, block, :] = jnp.dot(
            attended[block, :], weights[side], preferred_element_type=jnp.float32
        )

    def dest(side, s):
        return lax.rem(me + half + (s if side else n - s), n)

    def token(source, side, hop, u):
        piece = pl.ds(u * sub, sub)
        return pltpu.make_async_remote_copy(
            src_ref=source.at[piece, :],
            dst_ref=slots.at[side * half + hop, piece, :],
            send_sem=send_sem,
            recv_sem=(recv_left if side else recv_right).at[hop, u],
            device_id={"tp": left if side else right},
            device_id_type=MESH,
        )

    def slot(side, hop):
        return slots.at[side * half + hop]

    unpack(0, dest(0, 0))
    for i in range(2):
        multiply(0, 0, i)
    begun[...] = part[0, 0].astype(jnp.bfloat16)
    pl.semaphore_wait(barrier, 2)
    for u in range(pieces):
        token(begun, 2 * u // pieces, 0, u).start()
    for side in range(2):
        unpack(side, dest(side, 1))
        for i in range(2):
            multiply(side, 1, i)

    def ahead(s, turn, task):
        side = task % 2
        if task < 2:
            unpack(side, dest(side, s))
        else:
            multiply(side, turn, (task - 2) // 2)

    def step(s, joins):
        now, later = lax.rem(s, 2), lax.rem(s + 1, 2)
        for u in range(pieces):
            piece = pl.ds(u * sub, sub)
            for side in range(2):
                here = slot(side, s - 1)
                term = part[now, side, piece, :]
                if joins(side, u):
                    token(here, side, s - 1, u).wait_recv()
                    term = term + here[piece, :].astype(jnp.float32)
                here[piece, :] = term.astype(jnp.bfloat16)
                token(here, side, s, u).start()
            for task in range(6 * u // pieces, 6 * (u + 1) // pieces):
                ahead(s + 1, later, task)

    step(1, lambda side, u: side == 2 * u // pieces)

    @pl.loop(2, half)
    def _(s):
        step(s, lambda side, u: True)

    for u in range(pieces):
        piece = pl.ds(u * sub, sub)
        term = part[half % 2, 0, piece, :]
        for side in range(2):
            here = slot(side, half - 1)
            token(here, side, half - 1, u).wait_recv()
            term = term + here[piece, :].astype(jnp.float32)
        out_ref[piece, :] = term.astype(jnp.bfloat16)
    every = slots.at[pl.ds(0, n - 1)]
    pltpu.make_async_copy(every, every, send_sem).wait()


def prefill_kernel(page, pages_ref, q_ref, kv_ref, out_ref):
    rows = q_ref.shape[0]
    block = min(LONGEST, rows)
    for first in range(0, rows, block):
        low = max(0, first - LONGEST)
        count = first + block - low
        keys = kv_ref[low : first + block, 0:HD]
        values = kv_ref[low : first + block, HD:]
        row = lax.broadcasted_iota(jnp.int32, (block, count), 0) + first
        key = lax.broadcasted_iota(jnp.int32, (block, count), 1) + low
        start = prompt_start(pages_ref, page, row)
        allowed = (key <= row) & (key >= start)
        for lane in range(0, q_ref.shape[1], HD):
            query = q_ref[first : first + block, lane : lane + HD]
            scores = lax.dot_general(
                query, keys, (((1,), (1,)), ((), ())), preferred_element_type=jnp.float32
            ) * (HD**-0.5)
            scores = jnp.where(allowed, scores, -1e30)
            top = jnp.max(scores, axis=1, keepdims=True)
            raised = jnp.exp(scores - top)
            weight = raised * (1.0 / jnp.sum(raised, axis=1, keepdims=True))
            out_ref[first : first + block, lane : lane + HD] = jnp.dot(
                weight.astype(jnp.bfloat16), values, preferred_element_type=jnp.float32
            ).astype(jnp.bfloat16)


def decode_scratch(rows, width, tokens, pages, page):
    return [
        VMEM((pages, page, 2 * HD), jnp.bfloat16),
        VMEM((rows, width), jnp.float32),
        VMEM((rows, 2 * HD), jnp.float32),
        VMEM((2 * rows, tokens), jnp.float32),
        VMEM((2 * rows, HD), jnp.float32),
        VMEM((2 * rows, tokens), jnp.bfloat16),
        VMEM((rows, width), jnp.float32),
        pltpu.SemaphoreType.DMA,
    ]


def decode_kernel(
    table_ref, length_ref, q_ref, kv_ref, fresh_ref, pool_ref, out_ref,
    cache, q_wide, kv_wide, score_buf, self_buf, weight_buf, out_wide, load_sem,
):
    rows = q_ref.shape[0]
    pool, page, _ = pool_ref.shape
    span = table_ref.shape[0] // rows
    load = pltpu.make_async_copy(pool_ref, cache.at[pl.ds(0, pool)], load_sem)
    load.start()
    for j in range(rows // page):
        cache[pool + j] = fresh_ref[j * page : (j + 1) * page, :]
    q_wide[...] = q_ref[...].astype(jnp.float32)
    kv_wide[...] = kv_ref[...].astype(jnp.float32)
    load.wait()
    batch = 8
    owner = lax.rem(lax.broadcasted_iota(jnp.int32, (2 * batch, HD), 0), batch)
    spot = lax.broadcasted_iota(jnp.int32, (2 * batch, span * page), 1)

    def gathered(first, lane):
        pages = []
        for j in range(span):
            pair = [
                cache[table_ref[(first + t) * span + j], :, lane : lane + HD] for t in range(2)
            ]
            pages.append(jnp.concatenate(pair, axis=1))
        return jnp.concatenate(pages, axis=0)

    def twice(piece, ref, lane):
        return jnp.concatenate([ref[piece, lane : lane + HD]] * 2, axis=0)

    def score_block(b):
        first = pl.multiple_of(b * batch, batch)
        piece = pl.ds(first, batch)
        both = q_wide[piece, :]
        query = jnp.concatenate([both[:, 0:HD], both[:, HD:]], axis=0)
        length = jnp.concatenate([length_ref[piece, :]] * 2, axis=0)
        scores = None
        for p in range(0, batch, 2):
            mine = jnp.concatenate(
                [jnp.where(owner == p + t, query, 0.0) for t in range(2)], axis=1
            ).astype(jnp.bfloat16)
            term = lax.dot_general(
                mine, gathered(first + p, 0), (((1,), (1,)), ((), ())),
                preferred_element_type=jnp.float32,
            )
            scores = term if scores is None else scores + term
        out = pl.ds(2 * first, 2 * batch)
        score_buf[out, :] = jnp.where(spot < length, scores * (HD**-0.5), -1e30)
        self_score = jnp.sum(query * twice(piece, kv_wide, 0), axis=1, keepdims=True)
        self_buf[out, :] = jnp.broadcast_to(self_score * (HD**-0.5), (2 * batch, HD))

    def weigh(i):
        piece = pl.ds(i * 128, 128)
        scores, self_score = score_buf[piece, :], self_buf[piece, :]
        top = jnp.maximum(jnp.max(scores, axis=1, keepdims=True), self_score)
        raised = jnp.exp(scores - jnp.concatenate([top] * (scores.shape[1] // HD), axis=1))
        self_raised = jnp.exp(self_score - top)
        share = 1.0 / (jnp.sum(raised, axis=1, keepdims=True) + self_raised)
        share = jnp.broadcast_to(share, self_score.shape)
        weight_buf[piece, :] = (
            raised * jnp.concatenate([share] * (scores.shape[1] // HD), axis=1)
        ).astype(jnp.bfloat16)
        self_buf[piece, :] = (self_raised * share).astype(jnp.bfloat16).astype(jnp.float32)

    def value_block(b):
        first = pl.multiple_of(b * batch, batch)
        piece = pl.ds(first, batch)
        weight = weight_buf[pl.ds(2 * first, 2 * batch), :]
        total = self_buf[pl.ds(2 * first, 2 * batch), :] * twice(piece, kv_wide, HD)
        for p in range(0, batch, 2):
            term = jnp.dot(weight, gathered(first + p, HD), preferred_element_type=jnp.float32)
            for t in range(2):
                total = total + jnp.where(owner == p + t, term[:, t * HD : (t + 1) * HD], 0.0)
        out_wide[piece, 0:HD] = total[0:batch, :]
        out_wide[piece, HD:] = total[batch:, :]

    @pl.loop(0, rows // batch, step=4)
    def _(b):
        for i in range(4):
            score_block(b + i)

    @pl.loop(0, 2 * rows // 128)
    def _(i):
        weigh(i)

    @pl.loop(0, rows // batch, step=4)
    def _(b):
        for i in range(4):
            value_block(b + i)

    out_ref[...] = out_wide[...].astype(jnp.bfloat16)


def local(
    rows_in, norm_gain, q_words, q_scales, kv_words, kv_scales, o_words, o_scales,
    kv_pool, prompt_pages, page_slots, block_tables, cache_lens,
):
    n = lax.axis_size("tp")
    side = lax.axis_index("role")
    x = rows_in[0]
    rows, width = x.shape
    half = n // 2
    pool = kv_pool[0]
    page = pool.shape[1]
    count = prompt_pages.shape[0]
    dma = pltpu.SemaphoreType.DMA
    gather_sems, scatter_sems = dma((half, GATHER_PIECES)), dma((half, SCATTER_PIECES))
    in_vmem = pl.BlockSpec(memory_space=VMEM)
    in_smem = pl.BlockSpec(memory_space=pltpu.SMEM)
    in_hbm = pl.BlockSpec(memory_space=pltpu.HBM)
    bf16, f32 = jnp.bfloat16, jnp.float32

    lengths = jnp.concatenate([prompt_pages * page, cache_lens])
    freq = np.float32(500000.0) ** (-np.arange(HD // 2, dtype=np.float32) * 2 / HD)
    freq = jnp.asarray(np.concatenate([freq, freq])[None, :].astype(np.float32))

    half_block = jax.ShapeDtypeStruct((rows, width), bf16)
    query, fresh, arrived = pl.pallas_call(
        functools.partial(gather_project, page, n),
        out_shape=(
            half_block,
            jax.ShapeDtypeStruct((rows, 2 * HD), bf16),
            jax.ShapeDtypeStruct((rows, 2 * HD), bf16),
        ),
        in_specs=[in_smem] + [in_hbm] * 3 + [in_vmem] * 5,
        out_specs=(in_vmem, in_vmem, in_vmem),
        scratch_shapes=[
            VMEM((rows, width), bf16),
            VMEM((n, rows, width), bf16),
            VMEM((n, 1, rows), f32),
            VMEM((rows, width + 2 * HD), f32),
            VMEM((width, width + 2 * HD), bf16),
            VMEM((rows, 128), f32),
            VMEM((n, width), f32),
            VMEM((q_scales.shape[0], width + 2 * HD), f32),
            VMEM(q_words.shape, jnp.int32),
            VMEM(kv_words.shape[1:], jnp.int32),
            VMEM((rows, 2 * HD), bf16),
            VMEM((rows, HD), f32),
            VMEM((rows, HD), f32),
            dma((3,)), gather_sems, gather_sems, dma((half,)), dma((half,)),
            dma, dma, dma((2,)),
        ],
        compiler_params=pltpu.CompilerParams(
            collective_id=0, has_side_effects=True, vmem_limit_bytes=GATHER_VMEM
        ),
        cost_estimate=pl.CostEstimate(
            flops=4 * n * rows * width * width, bytes_accessed=4 << 20, transcendentals=0
        ),
        name="gather_project",
    )(
        prompt_pages, x, q_words, kv_words[0], q_scales, kv_scales[0],
        norm_gain.astype(f32).reshape(n, width), lengths.reshape(1, rows), freq,
    )

    def run_prefill():
        return pl.pallas_call(
            functools.partial(prefill_kernel, page),
            out_shape=half_block,
            in_specs=[in_smem] + [in_vmem] * 2,
            out_specs=in_vmem,
            name="prefill",
        )(prompt_pages, query, fresh)

    def run_decode():
        span = block_tables.shape[1]
        starts = jnp.cumsum(prompt_pages) - prompt_pages
        own = pool.shape[0] + jnp.minimum(
            starts[:, None] + jnp.arange(span, dtype=jnp.int32)[None, :],
            page_slots.shape[0] - 1,
        )
        table = jnp.concatenate([own, block_tables], axis=0).reshape(-1)
        return pl.pallas_call(
            decode_kernel,
            out_shape=half_block,
            in_specs=[in_smem] + [in_vmem] * 4 + [in_hbm],
            out_specs=in_vmem,
            scratch_shapes=decode_scratch(
                rows, width, span * page, pool.shape[0] + rows // page, page
            ),
            compiler_params=pltpu.CompilerParams(vmem_limit_bytes=24 << 20),
            name="decode",
        )(table, lengths[:, None], query, fresh, arrived, pool)

    attended = lax.cond(side == 0, run_prefill, run_decode)

    out = pl.pallas_call(
        functools.partial(project_scatter, n),
        out_shape=half_block,
        in_specs=[in_vmem, in_hbm, in_vmem],
        out_specs=in_vmem,
        scratch_shapes=[
            VMEM((rows, width), bf16),
            VMEM(o_words.shape, jnp.int32),
            VMEM((2, width, width), bf16),
            VMEM((2, 2, rows, width), f32),
            VMEM((rows, width), bf16),
            VMEM((n, rows, width), bf16),
            dma, scatter_sems, scatter_sems, dma,
        ],
        compiler_params=pltpu.CompilerParams(
            collective_id=1, has_side_effects=True, vmem_limit_bytes=40 << 20
        ),
        cost_estimate=pl.CostEstimate(
            flops=2 * n * rows * width * width, bytes_accessed=4 << 20, transcendentals=0
        ),
        name="project_scatter",
    )(attended, o_words, o_scales)
    return out[None]


def solution(mesh):
    return jax.shard_map(
        local,
        mesh=mesh,
        in_specs=(
            P("role", "groups", "tp"),
            P(),
            P(None, "tp"),
            P(None, "tp"),
            P("tp", None, None),
            P("tp", None, None),
            P("tp", None),
            P("tp", None),
            P("tp", "groups", None, None),
            P("groups"),
            P("groups"),
            P("groups", None),
            P("groups"),
        ),
        out_specs=P("role", "groups", "tp"),
        check_vma=False,
    )
```

```python
import functools

import jax
import jax.numpy as jnp
import numpy as np
from jax import lax
from jax.experimental import pallas as pl
from jax.experimental.pallas import tpu as pltpu
from jax.sharding import PartitionSpec as P

HD = 128
LONGEST = 128
GATHER_PIECES = 8
SCATTER_PIECES = 16
GATHER_VMEM = 58 << 20
MESH = pl.DeviceIdType.MESH
VMEM = pltpu.VMEM


def nibble_order(width):
    words = width // 8
    source = lax.broadcasted_iota(jnp.int32, (width, width), 0)
    column = lax.broadcasted_iota(jnp.int32, (width, width), 1)
    wanted = lax.rem(column, words) * 8 + column // words
    return jnp.where(source == wanted, 1.0, 0.0).astype(jnp.bfloat16)


def unpack_into(target, lane, words, low_scale, high_scale):
    count, width = words.shape
    half = count // 2
    scale = jnp.concatenate(
        [
            jnp.broadcast_to(low_scale, (half, width)),
            jnp.broadcast_to(high_scale, (half, width)),
        ],
        axis=0,
    )
    for k in range(8):
        nibble = jnp.bitwise_and(jnp.right_shift(words, 4 * k), 15) - 8
        value = (nibble.astype(jnp.float32) * scale).astype(jnp.bfloat16)
        target[k * count : (k + 1) * count, lane : lane + width] = value


def ring(n):
    me = lax.axis_index("tp")
    return me, lax.rem(me + 1, n), lax.rem(me + n - 1, n)


def signal_ready(peers):
    barrier = pltpu.get_barrier_semaphore()
    for peer in peers:
        pl.semaphore_signal(barrier, inc=1, device_id=peer, device_id_type=MESH)
    return barrier


def prompt_start(pages_ref, page, row):
    start, begin = jnp.zeros_like(row), 0
    for p in range(pages_ref.shape[0]):
        end = begin + pages_ref[p] * page
        start = jnp.where((row >= begin) & (row < end), begin, start)
        begin = end
    return start


def gather_project(
    page, n, pages_ref, length_ref, x_hbm, q_words, kv_words, q_scales, kv_scales, gain_ref,
    freq_ref, q_out, kv_out, fresh_out,
    x_ref, xbuf, stat, acc, weights, inverse, gains, scales, qw, kw, arrived, cosine, sine, held,
    load_sem, recv_right, recv_left, stat_right, stat_left, send_sem, stat_send, pair_sem,
):
    me, right, left = ring(n)
    role = lax.axis_index("role")
    half, turn = n // 2, n // 4
    rows, width = x_ref.shape
    pieces = recv_right.shape[1]
    sub = rows // pieces

    barrier = signal_ready(({"tp": right}, {"tp": left}, {"role": 1 - role}))
    load_x = pltpu.make_async_copy(x_hbm, x_ref, load_sem.at[0])
    loads = (
        pltpu.make_async_copy(q_words, qw, load_sem.at[1]),
        pltpu.make_async_copy(kv_words, kw, load_sem.at[2]),
    )
    load_x.start()
    for load in loads:
        load.start()

    order = nibble_order(width)
    load_x.wait()
    x = x_ref[...]
    xbuf[me] = jnp.dot(x, order, preferred_element_type=jnp.float32).astype(jnp.bfloat16)
    wide = x.astype(jnp.float32)
    squares = wide * wide
    folded = squares[:, 0:128]
    for lane in range(128, width, 128):
        folded = folded + squares[:, lane : lane + 128]
    stat[me] = jnp.sum(folded.T, axis=0, keepdims=True)

    def data(chunk, hop, u, to_right):
        piece = xbuf.at[chunk, pl.ds(u * sub, sub), :]
        return pltpu.make_async_remote_copy(
            src_ref=piece,
            dst_ref=piece,
            send_sem=send_sem,
            recv_sem=(recv_right if to_right else recv_left).at[hop, u],
            device_id={"tp": right if to_right else left},
            device_id_type=MESH,
        )

    def figure(chunk, hop, to_right):
        return pltpu.make_async_remote_copy(
            src_ref=stat.at[chunk],
            dst_ref=stat.at[chunk],
            send_sem=stat_send,
            recv_sem=(stat_right if to_right else stat_left).at[hop],
            device_id={"tp": right if to_right else left},
            device_id_type=MESH,
        )

    def behind(s):
        return lax.rem(me + n - s, n)

    def ahead(s):
        return lax.rem(me + s, n)

    def pass_figures(h):
        figure(behind(h), h - 1, True).wait_recv()
        figure(behind(h), h, True).start()
        figure(ahead(h), h - 1, False).wait_recv()
        figure(ahead(h), h, False).start()

    def pass_data(s, u):
        data(behind(s), s - 1, u, True).wait_recv()
        data(behind(s), s, u, True).start()
        data(ahead(s), s - 1, u, False).wait_recv()
        data(ahead(s), s, u, False).start()

    def project(chunk):
        low = scales[pl.ds(2 * chunk, 1), :]
        high = scales[pl.ds(2 * chunk + 1, 1), :]
        first = pl.multiple_of(chunk * (width // 8), width // 8)
        for lane, words in ((0, qw), (width, kw)):
            unpack_into(
                weights, lane, words[pl.ds(first, width // 8), :],
                low[:, lane : lane + width], high[:, lane : lane + width],
            )
        gain = gains[pl.ds(chunk, 1), :]
        for u in range(4):
            part = pl.ds(u * (rows // 4), rows // 4)
            scale = inverse[part, :]
            scale = jnp.concatenate([scale] * (width // 128), axis=1)
            normed = (xbuf[chunk, part, :].astype(jnp.float32) * scale * gain).astype(jnp.bfloat16)
            acc[part, :] += jnp.dot(normed, weights[...], preferred_element_type=jnp.float32)

    pl.semaphore_wait(barrier, 3)
    figure(me, 0, True).start()
    figure(me, 0, False).start()
    for u in range(pieces):
        data(me, 0, u, True).start()
        data(me, 0, u, False).start()
    gains[...] = jnp.dot(
        gain_ref[...], order, preferred_element_type=jnp.float32
    )
    scales[:, 0:width] = q_scales[...].astype(jnp.float32)
    scales[:, width:] = kv_scales[...].astype(jnp.float32)
    acc[...] = jnp.zeros_like(acc)
    row = lax.broadcasted_iota(jnp.int32, (rows, HD), 0)
    placed = (row - prompt_start(pages_ref, page, row)).astype(jnp.float32)
    prompts = pages_ref.shape[0]
    line = lax.broadcasted_iota(jnp.int32, (8, HD), 0)

    @pl.loop(0, rows // 8)
    def _(b):
        block = jnp.zeros((8, HD), jnp.int32)
        for t in range(8):
            i = 8 * b + t
            whole = pages_ref[jnp.minimum(i, prompts - 1)] * page
            length = jnp.where(i < prompts, whole, length_ref[jnp.maximum(i - prompts, 0)])
            block = jnp.where(line == t, length, block)
        held[pl.ds(pl.multiple_of(8 * b, 8), 8), :] = block.astype(jnp.float32)

    angle = jnp.where(role == 0, placed, held[...]) * freq_ref[...]
    cosine[...] = jnp.cos(angle)
    turned = jnp.sin(angle)
    lane = lax.broadcasted_iota(jnp.int32, (rows, HD), 1)
    sine[...] = jnp.where(lane < HD // 2, -turned, turned)
    for load in loads:
        load.wait()
    pass_figures(1)

    quarter = pieces // 4

    @pl.loop(1, turn)
    def _(s):
        for u in range(pieces):
            pass_data(s, u)
            if u == 2 * quarter - 1:
                pass_figures(2 * s)
            if u == pieces - 1:

                @pl.when(2 * s + 1 < half - 1)
                def _():
                    pass_figures(2 * s + 1)

                @pl.when(2 * s + 1 == half - 1)
                def _():
                    figure(behind(half - 1), half - 2, True).wait_recv()
                    figure(behind(half - 1), half - 1, True).start()
                    figure(ahead(half - 1), half - 2, False).wait_recv()

    figure(behind(half), half - 1, True).wait_recv()
    total = stat[0]
    for i in range(1, n):
        total = total + stat[i]
    mean = total / (n * width)
    inverse[...] = jnp.broadcast_to(lax.rsqrt(mean + 1e-05), (128, rows)).T

    @pl.loop(turn, half - 1)
    def _(s):
        for i in range(4):
            for u in range(i * quarter, (i + 1) * quarter):
                pass_data(s, u)
            o = 4 * (s - turn) + i
            project(behind((o + 1) // 2) if i % 2 else ahead(o // 2))

    last = half - 1
    for u in range(pieces):
        data(behind(last), last - 1, u, True).wait_recv()
        if u < pieces // 2:
            data(behind(last), last, u, True).start()
        data(ahead(last), last - 1, u, False).wait_recv()
        if u >= pieces // 2:
            data(ahead(last), last, u, False).start()
    project(ahead(last - 1))
    project(behind(last))
    project(ahead(last))
    for u in range(pieces):
        data(behind(half), last, u, u < pieces // 2).wait_recv()
    project(behind(half))

    def rotated(lane):
        head = acc[:, lane : lane + HD]
        turned = pltpu.roll(head, HD // 2, 1)
        return (head * cosine[...] + turned * sine[...]).astype(jnp.bfloat16)

    kv_out[:, 0:HD] = rotated(width)
    kv_out[:, HD:] = acc[:, width + HD :].astype(jnp.bfloat16)
    for lane in range(0, width, HD):
        q_out[:, lane : lane + HD] = rotated(lane)
    swap = pltpu.make_async_remote_copy(
        src_ref=kv_out, dst_ref=arrived, send_sem=pair_sem.at[0], recv_sem=pair_sem.at[1],
        device_id={"role": 1 - role}, device_id_type=MESH,
    )

    @pl.when(role == 0)
    def _():
        swap.start()
        fresh_out[...] = kv_out[...]
        swap.wait_send()

    @pl.when(role == 1)
    def _():
        swap.wait_recv()
        fresh_out[...] = arrived[...]

    every = xbuf.at[pl.ds(0, n - 1)]
    pltpu.make_async_copy(every, every, send_sem).wait()
    every = stat.at[pl.ds(0, n - 1)]
    pltpu.make_async_copy(every, every, stat_send).wait()


def project_scatter(
    n, att_ref, ow, scale_ref, out_ref,
    attended, weights, part, begun, slots, recv_right, recv_left, send_sem,
):
    me, right, left = ring(n)
    half = n // 2
    rows, width = att_ref.shape
    pieces = recv_right.shape[1]
    sub = rows // pieces
    barrier = signal_ready(({"tp": right}, {"tp": left}))
    attended[...] = jnp.dot(
        att_ref[...], nibble_order(width), preferred_element_type=jnp.float32
    ).astype(jnp.bfloat16)

    def unpack(side, dest):
        columns = pl.ds(pl.multiple_of(dest * width, width), width)
        scale = scale_ref[:, columns].astype(jnp.float32)
        unpack_into(weights.at[side], 0, ow[:, columns], scale[0:1, :], scale[1:2, :])

    def multiply(side, turn, i):
        block = pl.ds(i * (rows // 2), rows // 2)
        part[turn, side, block, :] = jnp.dot(
            attended[block, :], weights[side], preferred_element_type=jnp.float32
        )

    def dest(side, s):
        return lax.rem(me + half + (s if side else n - s), n)

    def token(source, side, hop, u):
        piece = pl.ds(u * sub, sub)
        return pltpu.make_async_remote_copy(
            src_ref=source.at[piece, :],
            dst_ref=slots.at[side * half + hop, piece, :],
            send_sem=send_sem,
            recv_sem=(recv_left if side else recv_right).at[hop, u],
            device_id={"tp": left if side else right},
            device_id_type=MESH,
        )

    def slot(side, hop):
        return slots.at[side * half + hop]

    unpack(0, dest(0, 0))
    for i in range(2):
        multiply(0, 0, i)
    begun[...] = part[0, 0].astype(jnp.bfloat16)
    pl.semaphore_wait(barrier, 2)
    for u in range(pieces):
        token(begun, 2 * u // pieces, 0, u).start()
    for side in range(2):
        unpack(side, dest(side, 1))
        for i in range(2):
            multiply(side, 1, i)

    def ahead(s, turn, task):
        side = task % 2
        if task < 2:
            unpack(side, dest(side, s))
        else:
            multiply(side, turn, (task - 2) // 2)

    def step(s, joins):
        now, later = lax.rem(s, 2), lax.rem(s + 1, 2)
        for u in range(pieces):
            piece = pl.ds(u * sub, sub)
            for side in range(2):
                here = slot(side, s - 1)
                term = part[now, side, piece, :]
                if joins(side, u):
                    token(here, side, s - 1, u).wait_recv()
                    term = term + here[piece, :].astype(jnp.float32)
                here[piece, :] = term.astype(jnp.bfloat16)
                token(here, side, s, u).start()
            for task in range(6 * u // pieces, 6 * (u + 1) // pieces):
                ahead(s + 1, later, task)

    step(1, lambda side, u: side == 2 * u // pieces)

    @pl.loop(2, half)
    def _(s):
        step(s, lambda side, u: True)

    for u in range(pieces):
        piece = pl.ds(u * sub, sub)
        term = part[half % 2, 0, piece, :]
        for side in range(2):
            here = slot(side, half - 1)
            token(here, side, half - 1, u).wait_recv()
            term = term + here[piece, :].astype(jnp.float32)
        out_ref[piece, :] = term.astype(jnp.bfloat16)
    every = slots.at[pl.ds(0, n - 1)]
    pltpu.make_async_copy(every, every, send_sem).wait()


def prefill_kernel(page, pages_ref, q_ref, kv_ref, out_ref):
    rows = q_ref.shape[0]
    block = min(LONGEST, rows)
    for first in range(0, rows, block):
        low = max(0, first - LONGEST)
        count = first + block - low
        keys = kv_ref[low : first + block, 0:HD]
        values = kv_ref[low : first + block, HD:]
        row = lax.broadcasted_iota(jnp.int32, (block, count), 0) + first
        key = lax.broadcasted_iota(jnp.int32, (block, count), 1) + low
        start = prompt_start(pages_ref, page, row)
        allowed = (key <= row) & (key >= start)
        for lane in range(0, q_ref.shape[1], HD):
            query = q_ref[first : first + block, lane : lane + HD]
            scores = lax.dot_general(
                query, keys, (((1,), (1,)), ((), ())), preferred_element_type=jnp.float32
            ) * (HD**-0.5)
            scores = jnp.where(allowed, scores, -1e30)
            top = jnp.max(scores, axis=1, keepdims=True)
            raised = jnp.exp(scores - top)
            weight = raised * (1.0 / jnp.sum(raised, axis=1, keepdims=True))
            out_ref[first : first + block, lane : lane + HD] = jnp.dot(
                weight.astype(jnp.bfloat16), values, preferred_element_type=jnp.float32
            ).astype(jnp.bfloat16)


def decode_scratch(rows, width, tokens, pages, page):
    return [
        VMEM((pages, page, 2 * HD), jnp.bfloat16),
        VMEM((rows, width), jnp.float32),
        VMEM((rows, 2 * HD), jnp.float32),
        VMEM((2 * rows, tokens), jnp.float32),
        VMEM((2 * rows, HD), jnp.float32),
        VMEM((2 * rows, tokens), jnp.bfloat16),
        VMEM((rows, width), jnp.float32),
        pltpu.SemaphoreType.DMA,
    ]


def decode_kernel(
    table_ref, length_ref, q_ref, kv_ref, fresh_ref, pool_ref, out_ref,
    cache, q_wide, kv_wide, score_buf, self_buf, weight_buf, out_wide, load_sem,
):
    rows = q_ref.shape[0]
    pool, page, _ = pool_ref.shape
    span = table_ref.shape[0] // rows
    load = pltpu.make_async_copy(pool_ref, cache.at[pl.ds(0, pool)], load_sem)
    load.start()
    for j in range(rows // page):
        cache[pool + j] = fresh_ref[j * page : (j + 1) * page, :]
    q_wide[...] = q_ref[...].astype(jnp.float32)
    kv_wide[...] = kv_ref[...].astype(jnp.float32)
    load.wait()
    batch = 8
    owner = lax.rem(lax.broadcasted_iota(jnp.int32, (2 * batch, HD), 0), batch)
    spot = lax.broadcasted_iota(jnp.int32, (2 * batch, span * page), 1)

    def gathered(first, lane):
        pages = []
        for j in range(span):
            pair = [
                cache[table_ref[(first + t) * span + j], :, lane : lane + HD] for t in range(2)
            ]
            pages.append(jnp.concatenate(pair, axis=1))
        return jnp.concatenate(pages, axis=0)

    def twice(piece, ref, lane):
        return jnp.concatenate([ref[piece, lane : lane + HD]] * 2, axis=0)

    def score_block(b):
        first = pl.multiple_of(b * batch, batch)
        piece = pl.ds(first, batch)
        both = q_wide[piece, :]
        query = jnp.concatenate([both[:, 0:HD], both[:, HD:]], axis=0)
        length = jnp.concatenate([length_ref[piece, :]] * 2, axis=0)
        scores = None
        for p in range(0, batch, 2):
            mine = jnp.concatenate(
                [jnp.where(owner == p + t, query, 0.0) for t in range(2)], axis=1
            ).astype(jnp.bfloat16)
            term = lax.dot_general(
                mine, gathered(first + p, 0), (((1,), (1,)), ((), ())),
                preferred_element_type=jnp.float32,
            )
            scores = term if scores is None else scores + term
        out = pl.ds(2 * first, 2 * batch)
        score_buf[out, :] = jnp.where(spot < length, scores * (HD**-0.5), -1e30)
        self_score = jnp.sum(query * twice(piece, kv_wide, 0), axis=1, keepdims=True)
        self_buf[out, :] = jnp.broadcast_to(self_score * (HD**-0.5), (2 * batch, HD))

    def weigh(i):
        piece = pl.ds(i * 128, 128)
        scores, self_score = score_buf[piece, :], self_buf[piece, :]
        top = jnp.maximum(jnp.max(scores, axis=1, keepdims=True), self_score)
        raised = jnp.exp(scores - jnp.concatenate([top] * (scores.shape[1] // HD), axis=1))
        self_raised = jnp.exp(self_score - top)
        share = 1.0 / (jnp.sum(raised, axis=1, keepdims=True) + self_raised)
        share = jnp.broadcast_to(share, self_score.shape)
        weight_buf[piece, :] = (
            raised * jnp.concatenate([share] * (scores.shape[1] // HD), axis=1)
        ).astype(jnp.bfloat16)
        self_buf[piece, :] = (self_raised * share).astype(jnp.bfloat16).astype(jnp.float32)

    def value_block(b):
        first = pl.multiple_of(b * batch, batch)
        piece = pl.ds(first, batch)
        weight = weight_buf[pl.ds(2 * first, 2 * batch), :]
        total = self_buf[pl.ds(2 * first, 2 * batch), :] * twice(piece, kv_wide, HD)
        for p in range(0, batch, 2):
            term = jnp.dot(weight, gathered(first + p, HD), preferred_element_type=jnp.float32)
            for t in range(2):
                total = total + jnp.where(owner == p + t, term[:, t * HD : (t + 1) * HD], 0.0)
        out_wide[piece, 0:HD] = total[0:batch, :]
        out_wide[piece, HD:] = total[batch:, :]

    @pl.loop(0, rows // batch, step=4)
    def _(b):
        for i in range(4):
            score_block(b + i)

    @pl.loop(0, 2 * rows // 128)
    def _(i):
        weigh(i)

    @pl.loop(0, rows // batch, step=4)
    def _(b):
        for i in range(4):
            value_block(b + i)

    out_ref[...] = out_wide[...].astype(jnp.bfloat16)


def local(
    rows_in, norm_gain, q_words, q_scales, kv_words, kv_scales, o_words, o_scales,
    kv_pool, prompt_pages, page_slots, block_tables, cache_lens,
):
    n = lax.axis_size("tp")
    side = lax.axis_index("role")
    x = rows_in[0]
    rows, width = x.shape
    half = n // 2
    pool = kv_pool[0]
    page = pool.shape[1]
    count = prompt_pages.shape[0]
    dma = pltpu.SemaphoreType.DMA
    gather_sems, scatter_sems = dma((half, GATHER_PIECES)), dma((half, SCATTER_PIECES))
    in_vmem = pl.BlockSpec(memory_space=VMEM)
    in_smem = pl.BlockSpec(memory_space=pltpu.SMEM)
    in_hbm = pl.BlockSpec(memory_space=pltpu.HBM)
    bf16, f32 = jnp.bfloat16, jnp.float32

    freq = np.float32(500000.0) ** (-np.arange(HD // 2, dtype=np.float32) * 2 / HD)
    freq = jnp.asarray(np.concatenate([freq, freq])[None, :].astype(np.float32))

    half_block = jax.ShapeDtypeStruct((rows, width), bf16)
    query, fresh, arrived = pl.pallas_call(
        functools.partial(gather_project, page, n),
        out_shape=(
            half_block,
            jax.ShapeDtypeStruct((rows, 2 * HD), bf16),
            jax.ShapeDtypeStruct((rows, 2 * HD), bf16),
        ),
        in_specs=[in_smem] * 2 + [in_hbm] * 3 + [in_vmem] * 4,
        out_specs=(in_vmem, in_vmem, in_vmem),
        scratch_shapes=[
            VMEM((rows, width), bf16),
            VMEM((n, rows, width), bf16),
            VMEM((n, 1, rows), f32),
            VMEM((rows, width + 2 * HD), f32),
            VMEM((width, width + 2 * HD), bf16),
            VMEM((rows, 128), f32),
            VMEM((n, width), f32),
            VMEM((q_scales.shape[0], width + 2 * HD), f32),
            VMEM(q_words.shape, jnp.int32),
            VMEM(kv_words.shape[1:], jnp.int32),
            VMEM((rows, 2 * HD), bf16),
            VMEM((rows, HD), f32),
            VMEM((rows, HD), f32),
            VMEM((rows, HD), f32),
            dma((3,)), gather_sems, gather_sems, dma((half,)), dma((half,)),
            dma, dma, dma((2,)),
        ],
        compiler_params=pltpu.CompilerParams(
            collective_id=0, has_side_effects=True, vmem_limit_bytes=GATHER_VMEM
        ),
        cost_estimate=pl.CostEstimate(
            flops=4 * n * rows * width * width, bytes_accessed=4 << 20, transcendentals=0
        ),
        name="gather_project",
    )(
        prompt_pages, cache_lens, x, q_words, kv_words[0], q_scales, kv_scales[0],
        norm_gain.reshape(n, width), freq,
    )

    def run_prefill():
        return pl.pallas_call(
            functools.partial(prefill_kernel, page),
            out_shape=half_block,
            in_specs=[in_smem] + [in_vmem] * 2,
            out_specs=in_vmem,
            name="prefill",
        )(prompt_pages, query, fresh)

    def run_decode():
        span = block_tables.shape[1]
        starts = jnp.cumsum(prompt_pages) - prompt_pages
        lengths = jnp.concatenate([prompt_pages * page, cache_lens])
        own = pool.shape[0] + jnp.minimum(
            starts[:, None] + jnp.arange(span, dtype=jnp.int32)[None, :],
            page_slots.shape[0] - 1,
        )
        table = jnp.concatenate([own, block_tables], axis=0).reshape(-1)
        return pl.pallas_call(
            decode_kernel,
            out_shape=half_block,
            in_specs=[in_smem] + [in_vmem] * 4 + [in_hbm],
            out_specs=in_vmem,
            scratch_shapes=decode_scratch(
                rows, width, span * page, pool.shape[0] + rows // page, page
            ),
            compiler_params=pltpu.CompilerParams(vmem_limit_bytes=24 << 20),
            name="decode",
        )(table, lengths[:, None], query, fresh, arrived, pool)

    attended = lax.cond(side == 0, run_prefill, run_decode)

    out = pl.pallas_call(
        functools.partial(project_scatter, n),
        out_shape=half_block,
        in_specs=[in_vmem] * 3,
        out_specs=in_vmem,
        scratch_shapes=[
            VMEM((rows, width), bf16),
            VMEM((2, width, width), bf16),
            VMEM((2, 2, rows, width), f32),
            VMEM((rows, width), bf16),
            VMEM((n, rows, width), bf16),
            scatter_sems, scatter_sems, dma,
        ],
        compiler_params=pltpu.CompilerParams(
            collective_id=1, has_side_effects=True, vmem_limit_bytes=40 << 20
        ),
        cost_estimate=pl.CostEstimate(
            flops=2 * n * rows * width * width, bytes_accessed=4 << 20, transcendentals=0
        ),
        name="project_scatter",
    )(attended, o_words, o_scales)
    return out[None]


def solution(mesh):
    return jax.shard_map(
        local,
        mesh=mesh,
        in_specs=(
            P("role", "groups", "tp"),
            P(),
            P(None, "tp"),
            P(None, "tp"),
            P("tp", None, None),
            P("tp", None, None),
            P("tp", None),
            P("tp", None),
            P("tp", "groups", None, None),
            P("groups"),
            P("groups"),
            P("groups", None),
            P("groups"),
        ),
        out_specs=P("role", "groups", "tp"),
        check_vma=False,
    )
```

```python
import functools

import jax
import jax.numpy as jnp
import numpy as np
from jax import lax
from jax.experimental import pallas as pl
from jax.experimental.pallas import tpu as pltpu
from jax.sharding import PartitionSpec as P

HD = 128
LONGEST = 128
GATHER_PIECES = 4
SCATTER_PIECES = 8
LEAD = 4
GATHER_VMEM = 58 << 20
MESH = pl.DeviceIdType.MESH
VMEM = pltpu.VMEM


def nibble_order(width):
    words = width // 8
    source = lax.broadcasted_iota(jnp.int32, (width, width), 0)
    column = lax.broadcasted_iota(jnp.int32, (width, width), 1)
    wanted = lax.rem(column, words) * 8 + column // words
    return jnp.where(source == wanted, 1.0, 0.0).astype(jnp.bfloat16)


def unpack_into(target, lane, words, low_scale, high_scale):
    count, width = words.shape
    half = count // 2
    scale = jnp.concatenate(
        [
            jnp.broadcast_to(low_scale, (half, width)),
            jnp.broadcast_to(high_scale, (half, width)),
        ],
        axis=0,
    )
    for k in range(8):
        nibble = jnp.bitwise_and(jnp.right_shift(words, 4 * k), 15) - 8
        value = (nibble.astype(jnp.float32) * scale).astype(jnp.bfloat16)
        target[k * count : (k + 1) * count, lane : lane + width] = value


def ring(n):
    me = lax.axis_index("tp")
    return me, lax.rem(me + 1, n), lax.rem(me + n - 1, n)


def signal_ready(peers):
    barrier = pltpu.get_barrier_semaphore()
    for peer in peers:
        pl.semaphore_signal(barrier, inc=1, device_id=peer, device_id_type=MESH)
    return barrier


def prompt_start(pages_ref, page, row):
    start, begin = jnp.zeros_like(row), 0
    for p in range(pages_ref.shape[0]):
        end = begin + pages_ref[p] * page
        start = jnp.where((row >= begin) & (row < end), begin, start)
        begin = end
    return start


def gather_project(
    page, n, pages_ref, length_ref, x_hbm, q_words, kv_words, q_scales, kv_scales, gain_ref,
    freq_ref, q_out, kv_out, fresh_out,
    x_ref, xbuf, stat, acc, weights, inverse, gains, scales, qw, kw, arrived, cosine, sine, held,
    load_sem, recv_right, recv_left, stat_right, stat_left, send_sem, stat_send, pair_sem, lead_sem,
):
    me, right, left = ring(n)
    role = lax.axis_index("role")
    half, turn = n // 2, n // 4
    rows, width = x_ref.shape
    pieces = recv_right.shape[1]
    sub = rows // pieces

    barrier = signal_ready(({"tp": right}, {"tp": left}, {"role": 1 - role}))
    load_x = pltpu.make_async_copy(x_hbm, x_ref, load_sem.at[0])
    loads = (
        pltpu.make_async_copy(q_words, qw, load_sem.at[1]),
        pltpu.make_async_copy(kv_words, kw, load_sem.at[2]),
    )
    load_x.start()
    for load in loads:
        load.start()

    order = nibble_order(width)
    load_x.wait()
    x = x_ref[...]
    xbuf[me] = jnp.dot(x, order, preferred_element_type=jnp.float32).astype(jnp.bfloat16)
    wide = x.astype(jnp.float32)
    squares = wide * wide
    folded = squares[:, 0:128]
    for lane in range(128, width, 128):
        folded = folded + squares[:, lane : lane + 128]
    stat[me] = jnp.sum(folded.T, axis=0, keepdims=True)

    def data(chunk, hop, u, to_right):
        piece = xbuf.at[chunk, pl.ds(u * sub, sub), :]
        return pltpu.make_async_remote_copy(
            src_ref=piece,
            dst_ref=piece,
            send_sem=send_sem,
            recv_sem=(recv_right if to_right else recv_left).at[hop, u],
            device_id={"tp": right if to_right else left},
            device_id_type=MESH,
        )

    def figure(chunk, hop, to_right):
        return pltpu.make_async_remote_copy(
            src_ref=stat.at[chunk],
            dst_ref=stat.at[chunk],
            send_sem=stat_send,
            recv_sem=(stat_right if to_right else stat_left).at[hop],
            device_id={"tp": right if to_right else left},
            device_id_type=MESH,
        )

    def behind(s):
        return lax.rem(me + n - s, n)

    def ahead(s):
        return lax.rem(me + s, n)

    def pass_figures(h):
        figure(behind(h), h - 1, True).wait_recv()
        figure(behind(h), h, True).start()
        figure(ahead(h), h - 1, False).wait_recv()
        figure(ahead(h), h, False).start()

    def pass_data(s, u):
        data(behind(s), s - 1, u, True).wait_recv()
        data(behind(s), s, u, True).start()
        data(ahead(s), s - 1, u, False).wait_recv()
        data(ahead(s), s, u, False).start()

    def project(chunk):
        low = scales[pl.ds(2 * chunk, 1), :]
        high = scales[pl.ds(2 * chunk + 1, 1), :]
        first = pl.multiple_of(chunk * (width // 8), width // 8)
        for lane, words in ((0, qw), (width, kw)):
            unpack_into(
                weights, lane, words[pl.ds(first, width // 8), :],
                low[:, lane : lane + width], high[:, lane : lane + width],
            )
        gain = gains[pl.ds(chunk, 1), :]
        for u in range(4):
            part = pl.ds(u * (rows // 4), rows // 4)
            scale = inverse[part, :]
            scale = jnp.concatenate([scale] * (width // 128), axis=1)
            normed = (xbuf[chunk, part, :].astype(jnp.float32) * scale * gain).astype(jnp.bfloat16)
            acc[part, :] += jnp.dot(normed, weights[...], preferred_element_type=jnp.float32)

    pl.semaphore_wait(barrier, 3)

    @pl.when(role == 1)
    def _():
        pl.semaphore_wait(lead_sem, 1)

    figure(me, 0, True).start()
    figure(me, 0, False).start()
    for u in range(pieces):
        data(me, 0, u, True).start()
        data(me, 0, u, False).start()
    for i in range(n):
        gains[i : i + 1, :] = gain_ref[i * width : (i + 1) * width].astype(jnp.float32)[None, :]
    gains[...] = jnp.dot(
        gains[...].astype(jnp.bfloat16), order, preferred_element_type=jnp.float32
    )
    scales[:, 0:width] = q_scales[...].astype(jnp.float32)
    scales[:, width:] = kv_scales[...].astype(jnp.float32)
    acc[...] = jnp.zeros_like(acc)
    row = lax.broadcasted_iota(jnp.int32, (rows, HD), 0)
    placed = (row - prompt_start(pages_ref, page, row)).astype(jnp.float32)
    prompts = pages_ref.shape[0]
    line = lax.broadcasted_iota(jnp.int32, (8, HD), 0)

    @pl.loop(0, rows // 8)
    def _(b):
        block = jnp.zeros((8, HD), jnp.int32)
        for t in range(8):
            i = 8 * b + t
            whole = pages_ref[jnp.minimum(i, prompts - 1)] * page
            length = jnp.where(i < prompts, whole, length_ref[jnp.maximum(i - prompts, 0)])
            block = jnp.where(line == t, length, block)
        held[pl.ds(pl.multiple_of(8 * b, 8), 8), :] = block.astype(jnp.float32)

    angle = jnp.where(role == 0, placed, held[...]) * freq_ref[...]
    cosine[...] = jnp.cos(angle)
    turned = jnp.sin(angle)
    lane = lax.broadcasted_iota(jnp.int32, (rows, HD), 1)
    sine[...] = jnp.where(lane < HD // 2, -turned, turned)
    for load in loads:
        load.wait()
    pass_figures(1)

    quarter = pieces // 4

    @pl.loop(1, turn)
    def _(s):
        @pl.when((role == 0) & (s == min(LEAD, turn - 1)))
        def _():
            pl.semaphore_signal(
                lead_sem, inc=1, device_id={"role": 1 - role}, device_id_type=MESH
            )

        for u in range(pieces):
            pass_data(s, u)
            if u == 2 * quarter - 1:
                pass_figures(2 * s)
            if u == pieces - 1:

                @pl.when(2 * s + 1 < half - 1)
                def _():
                    pass_figures(2 * s + 1)

                @pl.when(2 * s + 1 == half - 1)
                def _():
                    figure(behind(half - 1), half - 2, True).wait_recv()
                    figure(behind(half - 1), half - 1, True).start()
                    figure(ahead(half - 1), half - 2, False).wait_recv()

    figure(behind(half), half - 1, True).wait_recv()
    total = stat[0]
    for i in range(1, n):
        total = total + stat[i]
    mean = total / (n * width)
    inverse[...] = jnp.broadcast_to(lax.rsqrt(mean + 1e-05), (128, rows)).T

    @pl.loop(turn, half - 1)
    def _(s):
        for i in range(4):
            for u in range(i * quarter, (i + 1) * quarter):
                pass_data(s, u)
            o = 4 * (s - turn) + i
            project(behind((o + 1) // 2) if i % 2 else ahead(o // 2))

    last = half - 1
    for u in range(pieces):
        data(behind(last), last - 1, u, True).wait_recv()
        if u < pieces // 2:
            data(behind(last), last, u, True).start()
        data(ahead(last), last - 1, u, False).wait_recv()
        if u >= pieces // 2:
            data(ahead(last), last, u, False).start()
    project(ahead(last - 1))
    project(behind(last))
    project(ahead(last))
    for u in range(pieces):
        data(behind(half), last, u, u < pieces // 2).wait_recv()
    project(behind(half))

    def rotated(lane):
        head = acc[:, lane : lane + HD]
        turned = pltpu.roll(head, HD // 2, 1)
        return (head * cosine[...] + turned * sine[...]).astype(jnp.bfloat16)

    kv_out[:, 0:HD] = rotated(width)
    kv_out[:, HD:] = acc[:, width + HD :].astype(jnp.bfloat16)
    for lane in range(0, width, HD):
        q_out[:, lane : lane + HD] = rotated(lane)
    swap = pltpu.make_async_remote_copy(
        src_ref=kv_out, dst_ref=arrived, send_sem=pair_sem.at[0], recv_sem=pair_sem.at[1],
        device_id={"role": 1 - role}, device_id_type=MESH,
    )

    @pl.when(role == 0)
    def _():
        swap.start()
        fresh_out[...] = kv_out[...]
        swap.wait_send()

    @pl.when(role == 1)
    def _():
        swap.wait_recv()
        fresh_out[...] = arrived[...]

    every = xbuf.at[pl.ds(0, n - 1)]
    pltpu.make_async_copy(every, every, send_sem).wait()
    every = stat.at[pl.ds(0, n - 1)]
    pltpu.make_async_copy(every, every, stat_send).wait()


def project_scatter(
    n, att_ref, ow, scale_ref, out_ref,
    attended, weights, part, begun, slots, recv_right, recv_left, send_sem,
):
    me, right, left = ring(n)
    half = n // 2
    rows, width = att_ref.shape
    pieces = recv_right.shape[1]
    sub = rows // pieces
    barrier = signal_ready(({"tp": right}, {"tp": left}))
    attended[...] = jnp.dot(
        att_ref[...], nibble_order(width), preferred_element_type=jnp.float32
    ).astype(jnp.bfloat16)

    def unpack(side, dest):
        columns = pl.ds(pl.multiple_of(dest * width, width), width)
        scale = scale_ref[:, columns].astype(jnp.float32)
        unpack_into(weights.at[side], 0, ow[:, columns], scale[0:1, :], scale[1:2, :])

    def multiply(side, turn, i):
        block = pl.ds(i * (rows // 2), rows // 2)
        part[turn, side, block, :] = jnp.dot(
            attended[block, :], weights[side], preferred_element_type=jnp.float32
        )

    def dest(side, s):
        return lax.rem(me + half + (s if side else n - s), n)

    def token(source, side, hop, u):
        piece = pl.ds(u * sub, sub)
        return pltpu.make_async_remote_copy(
            src_ref=source.at[piece, :],
            dst_ref=slots.at[side * half + hop, piece, :],
            send_sem=send_sem,
            recv_sem=(recv_left if side else recv_right).at[hop, u],
            device_id={"tp": left if side else right},
            device_id_type=MESH,
        )

    def slot(side, hop):
        return slots.at[side * half + hop]

    unpack(0, dest(0, 0))
    for i in range(2):
        multiply(0, 0, i)
    begun[...] = part[0, 0].astype(jnp.bfloat16)
    pl.semaphore_wait(barrier, 2)
    for u in range(pieces):
        token(begun, 2 * u // pieces, 0, u).start()
    for side in range(2):
        unpack(side, dest(side, 1))
        for i in range(2):
            multiply(side, 1, i)

    def ahead(s, turn, task):
        side = task % 2
        if task < 2:
            unpack(side, dest(side, s))
        else:
            multiply(side, turn, (task - 2) // 2)

    def step(s, joins):
        now, later = lax.rem(s, 2), lax.rem(s + 1, 2)
        for u in range(pieces):
            piece = pl.ds(u * sub, sub)
            for side in range(2):
                here = slot(side, s - 1)
                term = part[now, side, piece, :]
                if joins(side, u):
                    token(here, side, s - 1, u).wait_recv()
                    term = term + here[piece, :].astype(jnp.float32)
                here[piece, :] = term.astype(jnp.bfloat16)
                token(here, side, s, u).start()
            for task in range(6 * u // pieces, 6 * (u + 1) // pieces):
                ahead(s + 1, later, task)

    step(1, lambda side, u: side == 2 * u // pieces)

    @pl.loop(2, half)
    def _(s):
        step(s, lambda side, u: True)

    for u in range(pieces):
        piece = pl.ds(u * sub, sub)
        term = part[half % 2, 0, piece, :]
        for side in range(2):
            here = slot(side, half - 1)
            token(here, side, half - 1, u).wait_recv()
            term = term + here[piece, :].astype(jnp.float32)
        out_ref[piece, :] = term.astype(jnp.bfloat16)
    every = slots.at[pl.ds(0, n - 1)]
    pltpu.make_async_copy(every, every, send_sem).wait()


def prefill_kernel(page, pages_ref, q_ref, kv_ref, out_ref):
    rows = q_ref.shape[0]
    block = min(LONGEST, rows)
    for first in range(0, rows, block):
        low = max(0, first - LONGEST)
        count = first + block - low
        keys = kv_ref[low : first + block, 0:HD]
        values = kv_ref[low : first + block, HD:]
        row = lax.broadcasted_iota(jnp.int32, (block, count), 0) + first
        key = lax.broadcasted_iota(jnp.int32, (block, count), 1) + low
        start = prompt_start(pages_ref, page, row)
        allowed = (key <= row) & (key >= start)
        for lane in range(0, q_ref.shape[1], HD):
            query = q_ref[first : first + block, lane : lane + HD]
            scores = lax.dot_general(
                query, keys, (((1,), (1,)), ((), ())), preferred_element_type=jnp.float32
            ) * (HD**-0.5)
            scores = jnp.where(allowed, scores, -1e30)
            top = jnp.max(scores, axis=1, keepdims=True)
            raised = jnp.exp(scores - top)
            weight = raised * (1.0 / jnp.sum(raised, axis=1, keepdims=True))
            out_ref[first : first + block, lane : lane + HD] = jnp.dot(
                weight.astype(jnp.bfloat16), values, preferred_element_type=jnp.float32
            ).astype(jnp.bfloat16)


def decode_scratch(rows, width, tokens, pages, page):
    return [
        VMEM((pages, page, 2 * HD), jnp.bfloat16),
        VMEM((rows, width), jnp.float32),
        VMEM((rows, 2 * HD), jnp.float32),
        VMEM((2 * rows, tokens), jnp.float32),
        VMEM((2 * rows, HD), jnp.float32),
        VMEM((2 * rows, tokens), jnp.bfloat16),
        VMEM((rows, width), jnp.float32),
        pltpu.SemaphoreType.DMA,
    ]


def decode_kernel(
    table_ref, length_ref, q_ref, kv_ref, fresh_ref, pool_ref, out_ref,
    cache, q_wide, kv_wide, score_buf, self_buf, weight_buf, out_wide, load_sem,
):
    rows = q_ref.shape[0]
    pool, page, _ = pool_ref.shape
    span = table_ref.shape[0] // rows
    load = pltpu.make_async_copy(pool_ref, cache.at[pl.ds(0, pool)], load_sem)
    load.start()
    for j in range(rows // page):
        cache[pool + j] = fresh_ref[j * page : (j + 1) * page, :]
    q_wide[...] = q_ref[...].astype(jnp.float32)
    kv_wide[...] = kv_ref[...].astype(jnp.float32)
    load.wait()
    batch = 8
    owner = lax.rem(lax.broadcasted_iota(jnp.int32, (2 * batch, HD), 0), batch)
    spot = lax.broadcasted_iota(jnp.int32, (2 * batch, span * page), 1)

    def gathered(first, lane):
        pages = []
        for j in range(span):
            pair = [
                cache[table_ref[(first + t) * span + j], :, lane : lane + HD] for t in range(2)
            ]
            pages.append(jnp.concatenate(pair, axis=1))
        return jnp.concatenate(pages, axis=0)

    def twice(piece, ref, lane):
        return jnp.concatenate([ref[piece, lane : lane + HD]] * 2, axis=0)

    def score_block(b):
        first = pl.multiple_of(b * batch, batch)
        piece = pl.ds(first, batch)
        both = q_wide[piece, :]
        query = jnp.concatenate([both[:, 0:HD], both[:, HD:]], axis=0)
        length = jnp.concatenate([length_ref[piece, :]] * 2, axis=0)
        scores = None
        for p in range(0, batch, 2):
            mine = jnp.concatenate(
                [jnp.where(owner == p + t, query, 0.0) for t in range(2)], axis=1
            ).astype(jnp.bfloat16)
            term = lax.dot_general(
                mine, gathered(first + p, 0), (((1,), (1,)), ((), ())),
                preferred_element_type=jnp.float32,
            )
            scores = term if scores is None else scores + term
        out = pl.ds(2 * first, 2 * batch)
        score_buf[out, :] = jnp.where(spot < length, scores * (HD**-0.5), -1e30)
        self_score = jnp.sum(query * twice(piece, kv_wide, 0), axis=1, keepdims=True)
        self_buf[out, :] = jnp.broadcast_to(self_score * (HD**-0.5), (2 * batch, HD))

    def weigh(i):
        piece = pl.ds(i * 128, 128)
        scores, self_score = score_buf[piece, :], self_buf[piece, :]
        top = jnp.maximum(jnp.max(scores, axis=1, keepdims=True), self_score)
        raised = jnp.exp(scores - jnp.concatenate([top] * (scores.shape[1] // HD), axis=1))
        self_raised = jnp.exp(self_score - top)
        share = 1.0 / (jnp.sum(raised, axis=1, keepdims=True) + self_raised)
        share = jnp.broadcast_to(share, self_score.shape)
        weight_buf[piece, :] = (
            raised * jnp.concatenate([share] * (scores.shape[1] // HD), axis=1)
        ).astype(jnp.bfloat16)
        self_buf[piece, :] = (self_raised * share).astype(jnp.bfloat16).astype(jnp.float32)

    def value_block(b):
        first = pl.multiple_of(b * batch, batch)
        piece = pl.ds(first, batch)
        weight = weight_buf[pl.ds(2 * first, 2 * batch), :]
        total = self_buf[pl.ds(2 * first, 2 * batch), :] * twice(piece, kv_wide, HD)
        for p in range(0, batch, 2):
            term = jnp.dot(weight, gathered(first + p, HD), preferred_element_type=jnp.float32)
            for t in range(2):
                total = total + jnp.where(owner == p + t, term[:, t * HD : (t + 1) * HD], 0.0)
        out_wide[piece, 0:HD] = total[0:batch, :]
        out_wide[piece, HD:] = total[batch:, :]

    @pl.loop(0, rows // batch, step=4)
    def _(b):
        for i in range(4):
            score_block(b + i)

    @pl.loop(0, 2 * rows // 128)
    def _(i):
        weigh(i)

    @pl.loop(0, rows // batch, step=4)
    def _(b):
        for i in range(4):
            value_block(b + i)

    out_ref[...] = out_wide[...].astype(jnp.bfloat16)


def local(
    rows_in, norm_gain, q_words, q_scales, kv_words, kv_scales, o_words, o_scales,
    kv_pool, prompt_pages, page_slots, block_tables, cache_lens,
):
    n = lax.axis_size("tp")
    side = lax.axis_index("role")
    x = rows_in[0]
    rows, width = x.shape
    half = n // 2
    pool = kv_pool[0]
    page = pool.shape[1]
    count = prompt_pages.shape[0]
    dma = pltpu.SemaphoreType.DMA
    gather_sems, scatter_sems = dma((half, GATHER_PIECES)), dma((half, SCATTER_PIECES))
    in_vmem = pl.BlockSpec(memory_space=VMEM)
    in_smem = pl.BlockSpec(memory_space=pltpu.SMEM)
    in_hbm = pl.BlockSpec(memory_space=pltpu.HBM)
    bf16, f32 = jnp.bfloat16, jnp.float32

    freq = np.float32(500000.0) ** (-np.arange(HD // 2, dtype=np.float32) * 2 / HD)
    freq = jnp.asarray(np.concatenate([freq, freq])[None, :].astype(np.float32))

    half_block = jax.ShapeDtypeStruct((rows, width), bf16)
    query, fresh, arrived = pl.pallas_call(
        functools.partial(gather_project, page, n),
        out_shape=(
            half_block,
            jax.ShapeDtypeStruct((rows, 2 * HD), bf16),
            jax.ShapeDtypeStruct((rows, 2 * HD), bf16),
        ),
        in_specs=[in_smem] * 2 + [in_hbm] * 3 + [in_vmem] * 4,
        out_specs=(in_vmem, in_vmem, in_vmem),
        scratch_shapes=[
            VMEM((rows, width), bf16),
            VMEM((n, rows, width), bf16),
            VMEM((n, 1, rows), f32),
            VMEM((rows, width + 2 * HD), f32),
            VMEM((width, width + 2 * HD), bf16),
            VMEM((rows, 128), f32),
            VMEM((n, width), f32),
            VMEM((q_scales.shape[0], width + 2 * HD), f32),
            VMEM(q_words.shape, jnp.int32),
            VMEM(kv_words.shape[1:], jnp.int32),
            VMEM((rows, 2 * HD), bf16),
            VMEM((rows, HD), f32),
            VMEM((rows, HD), f32),
            VMEM((rows, HD), f32),
            dma((3,)), gather_sems, gather_sems, dma((half,)), dma((half,)),
            dma, dma, dma((2,)), pltpu.SemaphoreType.REGULAR,
        ],
        compiler_params=pltpu.CompilerParams(
            collective_id=0, has_side_effects=True, vmem_limit_bytes=GATHER_VMEM
        ),
        cost_estimate=pl.CostEstimate(
            flops=4 * n * rows * width * width, bytes_accessed=4 << 20, transcendentals=0
        ),
        name="gather_project",
    )(
        prompt_pages, cache_lens, x, q_words, kv_words[0], q_scales, kv_scales[0],
        norm_gain, freq,
    )

    def run_prefill():
        return pl.pallas_call(
            functools.partial(prefill_kernel, page),
            out_shape=half_block,
            in_specs=[in_smem] + [in_vmem] * 2,
            out_specs=in_vmem,
            name="prefill",
        )(prompt_pages, query, fresh)

    def run_decode():
        span = block_tables.shape[1]
        starts = jnp.cumsum(prompt_pages) - prompt_pages
        lengths = jnp.concatenate([prompt_pages * page, cache_lens])
        own = pool.shape[0] + jnp.minimum(
            starts[:, None] + jnp.arange(span, dtype=jnp.int32)[None, :],
            page_slots.shape[0] - 1,
        )
        table = jnp.concatenate([own, block_tables], axis=0).reshape(-1)
        return pl.pallas_call(
            decode_kernel,
            out_shape=half_block,
            in_specs=[in_smem] + [in_vmem] * 4 + [in_hbm],
            out_specs=in_vmem,
            scratch_shapes=decode_scratch(
                rows, width, span * page, pool.shape[0] + rows // page, page
            ),
            compiler_params=pltpu.CompilerParams(vmem_limit_bytes=24 << 20),
            name="decode",
        )(table, lengths[:, None], query, fresh, arrived, pool)

    attended = lax.cond(side == 0, run_prefill, run_decode)

    out = pl.pallas_call(
        functools.partial(project_scatter, n),
        out_shape=half_block,
        in_specs=[in_vmem] * 3,
        out_specs=in_vmem,
        scratch_shapes=[
            VMEM((rows, width), bf16),
            VMEM((2, width, width), bf16),
            VMEM((2, 2, rows, width), f32),
            VMEM((rows, width), bf16),
            VMEM((n, rows, width), bf16),
            scatter_sems, scatter_sems, dma,
        ],
        compiler_params=pltpu.CompilerParams(
            collective_id=1, has_side_effects=True, vmem_limit_bytes=40 << 20
        ),
        cost_estimate=pl.CostEstimate(
            flops=2 * n * rows * width * width, bytes_accessed=4 << 20, transcendentals=0
        ),
        name="project_scatter",
    )(attended, o_words, o_scales)
    return out[None]


def solution(mesh):
    return jax.shard_map(
        local,
        mesh=mesh,
        in_specs=(
            P("role", "groups", "tp"),
            P(),
            P(None, "tp"),
            P(None, "tp"),
            P("tp", None, None),
            P("tp", None, None),
            P("tp", None),
            P("tp", None),
            P("tp", "groups", None, None),
            P("groups"),
            P("groups"),
            P("groups", None),
            P("groups"),
        ),
        out_specs=P("role", "groups", "tp"),
        check_vma=False,
    )
```

```python
import functools

import jax
import jax.numpy as jnp
import numpy as np
from jax import lax
from jax.experimental import pallas as pl
from jax.experimental.pallas import tpu as pltpu
from jax.sharding import PartitionSpec as P

HD = 128
LONGEST = 128
GATHER_PIECES = 4
SCATTER_PIECES = 8
REACH = 4
LEAD = 4
GATHER_VMEM = 58 << 20
MESH = pl.DeviceIdType.MESH
VMEM = pltpu.VMEM


def nibble_order(width):
    words = width // 8
    source = lax.broadcasted_iota(jnp.int32, (width, width), 0)
    column = lax.broadcasted_iota(jnp.int32, (width, width), 1)
    wanted = lax.rem(column, words) * 8 + column // words
    return jnp.where(source == wanted, 1.0, 0.0).astype(jnp.bfloat16)


def unpack_into(target, lane, words, low_scale, high_scale):
    count, width = words.shape
    half = count // 2
    scale = jnp.concatenate(
        [
            jnp.broadcast_to(low_scale, (half, width)),
            jnp.broadcast_to(high_scale, (half, width)),
        ],
        axis=0,
    )
    for k in range(8):
        nibble = jnp.bitwise_and(jnp.right_shift(words, 4 * k), 15) - 8
        value = (nibble.astype(jnp.float32) * scale).astype(jnp.bfloat16)
        target[k * count : (k + 1) * count, lane : lane + width] = value


def ring(n):
    me = lax.axis_index("tp")
    return me, lax.rem(me + 1, n), lax.rem(me + n - 1, n)


def signal_ready(peers):
    barrier = pltpu.get_barrier_semaphore()
    for peer in peers:
        pl.semaphore_signal(barrier, inc=1, device_id=peer, device_id_type=MESH)
    return barrier


def prompt_start(pages_ref, page, row):
    start, begin = jnp.zeros_like(row), 0
    for p in range(pages_ref.shape[0]):
        end = begin + pages_ref[p] * page
        start = jnp.where((row >= begin) & (row < end), begin, start)
        begin = end
    return start


def gather_project(
    page, n, pages_ref, length_ref, x_hbm, q_words, kv_words, q_scales, kv_scales, gain_ref,
    freq_ref, q_out, kv_out, fresh_out,
    x_ref, xbuf, stat, acc, weights, inverse, gains, scales, qw, kw, arrived, cosine, sine, held,
    load_sem, recv_right, recv_left, stat_right, stat_left, send_sem, stat_send, pair_sem, lead_sem,
):
    me, right, left = ring(n)
    role = lax.axis_index("role")
    half, turn = n // 2, n // 4
    rows, width = x_ref.shape
    pieces = recv_right.shape[1]
    sub = rows // pieces

    reach = min(REACH, half)
    groups = half // reach

    def behind(s):
        return lax.rem(me + n - s, n)

    def ahead(s):
        return lax.rem(me + s, n)

    peers = [{"tp": side(d)} for d in range(1, reach + 1) for side in (ahead, behind)]
    barrier = signal_ready(peers + [{"role": 1 - role}])
    load_x = pltpu.make_async_copy(x_hbm, x_ref, load_sem.at[0])
    loads = (
        pltpu.make_async_copy(q_words, qw, load_sem.at[1]),
        pltpu.make_async_copy(kv_words, kw, load_sem.at[2]),
    )
    load_x.start()
    for load in loads:
        load.start()

    order = nibble_order(width)
    load_x.wait()
    x = x_ref[...]
    xbuf[me] = jnp.dot(x, order, preferred_element_type=jnp.float32).astype(jnp.bfloat16)
    wide = x.astype(jnp.float32)
    squares = wide * wide
    folded = squares[:, 0:128]
    for lane in range(128, width, 128):
        folded = folded + squares[:, lane : lane + 128]
    stat[me] = jnp.sum(folded.T, axis=0, keepdims=True)

    def data(chunk, hop, u, to_right):
        piece = xbuf.at[chunk, pl.ds(u * sub, sub), :]
        return pltpu.make_async_remote_copy(
            src_ref=piece,
            dst_ref=piece,
            send_sem=send_sem,
            recv_sem=(recv_right if to_right else recv_left).at[hop, u],
            device_id={"tp": right if to_right else left},
            device_id_type=MESH,
        )

    def figure(chunk, sem, peer):
        return pltpu.make_async_remote_copy(
            src_ref=stat.at[chunk],
            dst_ref=stat.at[chunk],
            send_sem=stat_send,
            recv_sem=sem,
            device_id={"tp": peer},
            device_id_type=MESH,
        )

    def take_figures(g):
        for d in range(1, reach + 1):
            k = reach * (g - 1) + d
            figure(behind(k), stat_right.at[k - 1], right).wait_recv()

            @pl.when(k < half)
            def _():
                figure(ahead(k), stat_left.at[k - 1], left).wait_recv()

    def hand_on_figures(g):
        for d in range(1, reach + 1):
            k = reach * (g - 1) + d
            figure(behind(k), stat_right.at[k + reach - 1], ahead(reach)).start()

            @pl.when(k + reach < half)
            def _():
                figure(ahead(k), stat_left.at[k + reach - 1], behind(reach)).start()

    def pass_data(s, u):
        data(behind(s), s - 1, u, True).wait_recv()
        data(behind(s), s, u, True).start()
        data(ahead(s), s - 1, u, False).wait_recv()
        data(ahead(s), s, u, False).start()

    def project(chunk):
        low = scales[pl.ds(2 * chunk, 1), :]
        high = scales[pl.ds(2 * chunk + 1, 1), :]
        first = pl.multiple_of(chunk * (width // 8), width // 8)
        for lane, words in ((0, qw), (width, kw)):
            unpack_into(
                weights, lane, words[pl.ds(first, width // 8), :],
                low[:, lane : lane + width], high[:, lane : lane + width],
            )
        gain = gains[pl.ds(chunk, 1), :]
        for u in range(4):
            part = pl.ds(u * (rows // 4), rows // 4)
            scale = inverse[part, :]
            scale = jnp.concatenate([scale] * (width // 128), axis=1)
            normed = (xbuf[chunk, part, :].astype(jnp.float32) * scale * gain).astype(jnp.bfloat16)
            acc[part, :] += jnp.dot(normed, weights[...], preferred_element_type=jnp.float32)

    pl.semaphore_wait(barrier, 2 * reach + 1)

    @pl.when(role == 1)
    def _():
        pl.semaphore_wait(lead_sem, 1)

    for d in range(1, reach + 1):
        figure(me, stat_right.at[d - 1], ahead(d)).start()
        if d < half:
            figure(me, stat_left.at[d - 1], behind(d)).start()
    for u in range(pieces):
        data(me, 0, u, True).start()
        data(me, 0, u, False).start()
    for i in range(n):
        gains[i : i + 1, :] = gain_ref[i * width : (i + 1) * width].astype(jnp.float32)[None, :]
    gains[...] = jnp.dot(
        gains[...].astype(jnp.bfloat16), order, preferred_element_type=jnp.float32
    )
    scales[:, 0:width] = q_scales[...].astype(jnp.float32)
    scales[:, width:] = kv_scales[...].astype(jnp.float32)
    acc[...] = jnp.zeros_like(acc)
    row = lax.broadcasted_iota(jnp.int32, (rows, HD), 0)
    placed = (row - prompt_start(pages_ref, page, row)).astype(jnp.float32)
    prompts = pages_ref.shape[0]
    line = lax.broadcasted_iota(jnp.int32, (8, HD), 0)

    @pl.loop(0, rows // 8)
    def _(b):
        block = jnp.zeros((8, HD), jnp.int32)
        for t in range(8):
            i = 8 * b + t
            whole = pages_ref[jnp.minimum(i, prompts - 1)] * page
            length = jnp.where(i < prompts, whole, length_ref[jnp.maximum(i - prompts, 0)])
            block = jnp.where(line == t, length, block)
        held[pl.ds(pl.multiple_of(8 * b, 8), 8), :] = block.astype(jnp.float32)

    angle = jnp.where(role == 0, placed, held[...]) * freq_ref[...]
    cosine[...] = jnp.cos(angle)
    turned = jnp.sin(angle)
    lane = lax.broadcasted_iota(jnp.int32, (rows, HD), 1)
    sine[...] = jnp.where(lane < HD // 2, -turned, turned)
    for load in loads:
        load.wait()

    quarter = pieces // 4

    @pl.loop(1, turn)
    def _(s):
        @pl.when((role == 0) & (s == min(LEAD, turn - 1)))
        def _():
            pl.semaphore_signal(
                lead_sem, inc=1, device_id={"role": 1 - role}, device_id_type=MESH
            )

        for u in range(pieces):
            pass_data(s, u)
        group = (s + 1) // 2

        @pl.when((lax.rem(s, 2) == 1) & (group < groups))
        def _():
            take_figures(group)
            hand_on_figures(group)

    take_figures(groups)
    total = stat[0]
    for i in range(1, n):
        total = total + stat[i]
    mean = total / (n * width)
    inverse[...] = jnp.broadcast_to(lax.rsqrt(mean + 1e-05), (128, rows)).T

    @pl.loop(turn, half - 1)
    def _(s):
        for i in range(4):
            for u in range(i * quarter, (i + 1) * quarter):
                pass_data(s, u)
            o = 4 * (s - turn) + i
            project(behind((o + 1) // 2) if i % 2 else ahead(o // 2))

    last = half - 1
    for u in range(pieces):
        data(behind(last), last - 1, u, True).wait_recv()
        if u < pieces // 2:
            data(behind(last), last, u, True).start()
        data(ahead(last), last - 1, u, False).wait_recv()
        if u >= pieces // 2:
            data(ahead(last), last, u, False).start()
    project(ahead(last - 1))
    project(behind(last))
    project(ahead(last))
    for u in range(pieces):
        data(behind(half), last, u, u < pieces // 2).wait_recv()
    project(behind(half))

    def rotated(lane):
        head = acc[:, lane : lane + HD]
        turned = pltpu.roll(head, HD // 2, 1)
        return (head * cosine[...] + turned * sine[...]).astype(jnp.bfloat16)

    kv_out[:, 0:HD] = rotated(width)
    kv_out[:, HD:] = acc[:, width + HD :].astype(jnp.bfloat16)
    for lane in range(0, width, HD):
        q_out[:, lane : lane + HD] = rotated(lane)
    swap = pltpu.make_async_remote_copy(
        src_ref=kv_out, dst_ref=arrived, send_sem=pair_sem.at[0], recv_sem=pair_sem.at[1],
        device_id={"role": 1 - role}, device_id_type=MESH,
    )

    @pl.when(role == 0)
    def _():
        swap.start()
        fresh_out[...] = kv_out[...]
        swap.wait_send()

    @pl.when(role == 1)
    def _():
        swap.wait_recv()
        fresh_out[...] = arrived[...]

    every = xbuf.at[pl.ds(0, n - 1)]
    pltpu.make_async_copy(every, every, send_sem).wait()
    every = stat.at[pl.ds(0, n - 1)]
    pltpu.make_async_copy(every, every, stat_send).wait()


def project_scatter(
    n, att_ref, ow, scale_ref, out_ref,
    attended, weights, part, begun, slots, recv_right, recv_left, send_sem,
):
    me, right, left = ring(n)
    half = n // 2
    rows, width = att_ref.shape
    pieces = recv_right.shape[1]
    sub = rows // pieces
    barrier = signal_ready(({"tp": right}, {"tp": left}))
    attended[...] = jnp.dot(
        att_ref[...], nibble_order(width), preferred_element_type=jnp.float32
    ).astype(jnp.bfloat16)

    def unpack(side, dest):
        columns = pl.ds(pl.multiple_of(dest * width, width), width)
        scale = scale_ref[:, columns].astype(jnp.float32)
        unpack_into(weights.at[side], 0, ow[:, columns], scale[0:1, :], scale[1:2, :])

    def multiply(side, turn, i):
        block = pl.ds(i * (rows // 2), rows // 2)
        part[turn, side, block, :] = jnp.dot(
            attended[block, :], weights[side], preferred_element_type=jnp.float32
        )

    def dest(side, s):
        return lax.rem(me + half + (s if side else n - s), n)

    def token(source, side, hop, u):
        piece = pl.ds(u * sub, sub)
        return pltpu.make_async_remote_copy(
            src_ref=source.at[piece, :],
            dst_ref=slots.at[side * half + hop, piece, :],
            send_sem=send_sem,
            recv_sem=(recv_left if side else recv_right).at[hop, u],
            device_id={"tp": left if side else right},
            device_id_type=MESH,
        )

    def slot(side, hop):
        return slots.at[side * half + hop]

    unpack(0, dest(0, 0))
    for i in range(2):
        multiply(0, 0, i)
    begun[...] = part[0, 0].astype(jnp.bfloat16)
    pl.semaphore_wait(barrier, 2)
    for u in range(pieces):
        token(begun, 2 * u // pieces, 0, u).start()
    for side in range(2):
        unpack(side, dest(side, 1))
        for i in range(2):
            multiply(side, 1, i)

    def ahead(s, turn, task):
        side = task % 2
        if task < 2:
            unpack(side, dest(side, s))
        else:
            multiply(side, turn, (task - 2) // 2)

    def step(s, joins):
        now, later = lax.rem(s, 2), lax.rem(s + 1, 2)
        for u in range(pieces):
            piece = pl.ds(u * sub, sub)
            for side in range(2):
                here = slot(side, s - 1)
                term = part[now, side, piece, :]
                if joins(side, u):
                    token(here, side, s - 1, u).wait_recv()
                    term = term + here[piece, :].astype(jnp.float32)
                here[piece, :] = term.astype(jnp.bfloat16)
                token(here, side, s, u).start()
            for task in range(6 * u // pieces, 6 * (u + 1) // pieces):
                ahead(s + 1, later, task)

    step(1, lambda side, u: side == 2 * u // pieces)

    @pl.loop(2, half)
    def _(s):
        step(s, lambda side, u: True)

    for u in range(pieces):
        piece = pl.ds(u * sub, sub)
        term = part[half % 2, 0, piece, :]
        for side in range(2):
            here = slot(side, half - 1)
            token(here, side, half - 1, u).wait_recv()
            term = term + here[piece, :].astype(jnp.float32)
        out_ref[piece, :] = term.astype(jnp.bfloat16)
    every = slots.at[pl.ds(0, n - 1)]
    pltpu.make_async_copy(every, every, send_sem).wait()


def prefill_kernel(page, pages_ref, q_ref, kv_ref, out_ref):
    rows = q_ref.shape[0]
    block = min(LONGEST, rows)
    for first in range(0, rows, block):
        low = max(0, first - LONGEST)
        count = first + block - low
        keys = kv_ref[low : first + block, 0:HD]
        values = kv_ref[low : first + block, HD:]
        row = lax.broadcasted_iota(jnp.int32, (block, count), 0) + first
        key = lax.broadcasted_iota(jnp.int32, (block, count), 1) + low
        start = prompt_start(pages_ref, page, row)
        allowed = (key <= row) & (key >= start)
        for lane in range(0, q_ref.shape[1], HD):
            query = q_ref[first : first + block, lane : lane + HD]
            scores = lax.dot_general(
                query, keys, (((1,), (1,)), ((), ())), preferred_element_type=jnp.float32
            ) * (HD**-0.5)
            scores = jnp.where(allowed, scores, -1e30)
            top = jnp.max(scores, axis=1, keepdims=True)
            raised = jnp.exp(scores - top)
            weight = raised * (1.0 / jnp.sum(raised, axis=1, keepdims=True))
            out_ref[first : first + block, lane : lane + HD] = jnp.dot(
                weight.astype(jnp.bfloat16), values, preferred_element_type=jnp.float32
            ).astype(jnp.bfloat16)


def decode_scratch(rows, width, tokens, pages, page):
    return [
        VMEM((pages, page, 2 * HD), jnp.bfloat16),
        VMEM((rows, width), jnp.float32),
        VMEM((rows, 2 * HD), jnp.float32),
        VMEM((2 * rows, tokens), jnp.float32),
        VMEM((2 * rows, HD), jnp.float32),
        VMEM((2 * rows, tokens), jnp.bfloat16),
        VMEM((rows, width), jnp.float32),
        pltpu.SemaphoreType.DMA,
    ]


def decode_kernel(
    table_ref, length_ref, q_ref, kv_ref, fresh_ref, pool_ref, out_ref,
    cache, q_wide, kv_wide, score_buf, self_buf, weight_buf, out_wide, load_sem,
):
    rows = q_ref.shape[0]
    pool, page, _ = pool_ref.shape
    span = table_ref.shape[0] // rows
    load = pltpu.make_async_copy(pool_ref, cache.at[pl.ds(0, pool)], load_sem)
    load.start()
    for j in range(rows // page):
        cache[pool + j] = fresh_ref[j * page : (j + 1) * page, :]
    q_wide[...] = q_ref[...].astype(jnp.float32)
    kv_wide[...] = kv_ref[...].astype(jnp.float32)
    load.wait()
    batch = 8
    owner = lax.rem(lax.broadcasted_iota(jnp.int32, (2 * batch, HD), 0), batch)
    spot = lax.broadcasted_iota(jnp.int32, (2 * batch, span * page), 1)

    def gathered(first, lane):
        pages = []
        for j in range(span):
            pair = [
                cache[table_ref[(first + t) * span + j], :, lane : lane + HD] for t in range(2)
            ]
            pages.append(jnp.concatenate(pair, axis=1))
        return jnp.concatenate(pages, axis=0)

    def twice(piece, ref, lane):
        return jnp.concatenate([ref[piece, lane : lane + HD]] * 2, axis=0)

    def score_block(b):
        first = pl.multiple_of(b * batch, batch)
        piece = pl.ds(first, batch)
        both = q_wide[piece, :]
        query = jnp.concatenate([both[:, 0:HD], both[:, HD:]], axis=0)
        length = jnp.concatenate([length_ref[piece, :]] * 2, axis=0)
        scores = None
        for p in range(0, batch, 2):
            mine = jnp.concatenate(
                [jnp.where(owner == p + t, query, 0.0) for t in range(2)], axis=1
            ).astype(jnp.bfloat16)
            term = lax.dot_general(
                mine, gathered(first + p, 0), (((1,), (1,)), ((), ())),
                preferred_element_type=jnp.float32,
            )
            scores = term if scores is None else scores + term
        out = pl.ds(2 * first, 2 * batch)
        score_buf[out, :] = jnp.where(spot < length, scores * (HD**-0.5), -1e30)
        self_score = jnp.sum(query * twice(piece, kv_wide, 0), axis=1, keepdims=True)
        self_buf[out, :] = jnp.broadcast_to(self_score * (HD**-0.5), (2 * batch, HD))

    def weigh(i):
        piece = pl.ds(i * 128, 128)
        scores, self_score = score_buf[piece, :], self_buf[piece, :]
        top = jnp.maximum(jnp.max(scores, axis=1, keepdims=True), self_score)
        raised = jnp.exp(scores - jnp.concatenate([top] * (scores.shape[1] // HD), axis=1))
        self_raised = jnp.exp(self_score - top)
        share = 1.0 / (jnp.sum(raised, axis=1, keepdims=True) + self_raised)
        share = jnp.broadcast_to(share, self_score.shape)
        weight_buf[piece, :] = (
            raised * jnp.concatenate([share] * (scores.shape[1] // HD), axis=1)
        ).astype(jnp.bfloat16)
        self_buf[piece, :] = (self_raised * share).astype(jnp.bfloat16).astype(jnp.float32)

    def value_block(b):
        first = pl.multiple_of(b * batch, batch)
        piece = pl.ds(first, batch)
        weight = weight_buf[pl.ds(2 * first, 2 * batch), :]
        total = self_buf[pl.ds(2 * first, 2 * batch), :] * twice(piece, kv_wide, HD)
        for p in range(0, batch, 2):
            term = jnp.dot(weight, gathered(first + p, HD), preferred_element_type=jnp.float32)
            for t in range(2):
                total = total + jnp.where(owner == p + t, term[:, t * HD : (t + 1) * HD], 0.0)
        out_wide[piece, 0:HD] = total[0:batch, :]
        out_wide[piece, HD:] = total[batch:, :]

    @pl.loop(0, rows // batch, step=4)
    def _(b):
        for i in range(4):
            score_block(b + i)

    @pl.loop(0, 2 * rows // 128)
    def _(i):
        weigh(i)

    @pl.loop(0, rows // batch, step=4)
    def _(b):
        for i in range(4):
            value_block(b + i)

    out_ref[...] = out_wide[...].astype(jnp.bfloat16)


def local(
    rows_in, norm_gain, q_words, q_scales, kv_words, kv_scales, o_words, o_scales,
    kv_pool, prompt_pages, page_slots, block_tables, cache_lens,
):
    n = lax.axis_size("tp")
    side = lax.axis_index("role")
    x = rows_in[0]
    rows, width = x.shape
    half = n // 2
    pool = kv_pool[0]
    page = pool.shape[1]
    count = prompt_pages.shape[0]
    dma = pltpu.SemaphoreType.DMA
    gather_sems, scatter_sems = dma((half, GATHER_PIECES)), dma((half, SCATTER_PIECES))
    in_vmem = pl.BlockSpec(memory_space=VMEM)
    in_smem = pl.BlockSpec(memory_space=pltpu.SMEM)
    in_hbm = pl.BlockSpec(memory_space=pltpu.HBM)
    bf16, f32 = jnp.bfloat16, jnp.float32

    freq = np.float32(500000.0) ** (-np.arange(HD // 2, dtype=np.float32) * 2 / HD)
    freq = jnp.asarray(np.concatenate([freq, freq])[None, :].astype(np.float32))

    half_block = jax.ShapeDtypeStruct((rows, width), bf16)
    query, fresh, arrived = pl.pallas_call(
        functools.partial(gather_project, page, n),
        out_shape=(
            half_block,
            jax.ShapeDtypeStruct((rows, 2 * HD), bf16),
            jax.ShapeDtypeStruct((rows, 2 * HD), bf16),
        ),
        in_specs=[in_smem] * 2 + [in_hbm] * 3 + [in_vmem] * 4,
        out_specs=(in_vmem, in_vmem, in_vmem),
        scratch_shapes=[
            VMEM((rows, width), bf16),
            VMEM((n, rows, width), bf16),
            VMEM((n, 1, rows), f32),
            VMEM((rows, width + 2 * HD), f32),
            VMEM((width, width + 2 * HD), bf16),
            VMEM((rows, 128), f32),
            VMEM((n, width), f32),
            VMEM((q_scales.shape[0], width + 2 * HD), f32),
            VMEM(q_words.shape, jnp.int32),
            VMEM(kv_words.shape[1:], jnp.int32),
            VMEM((rows, 2 * HD), bf16),
            VMEM((rows, HD), f32),
            VMEM((rows, HD), f32),
            VMEM((rows, HD), f32),
            dma((3,)), gather_sems, gather_sems, dma((half,)), dma((half,)),
            dma, dma, dma((2,)), pltpu.SemaphoreType.REGULAR,
        ],
        compiler_params=pltpu.CompilerParams(
            collective_id=0, has_side_effects=True, vmem_limit_bytes=GATHER_VMEM
        ),
        cost_estimate=pl.CostEstimate(
            flops=4 * n * rows * width * width, bytes_accessed=4 << 20, transcendentals=0
        ),
        name="gather_project",
    )(
        prompt_pages, cache_lens, x, q_words, kv_words[0], q_scales, kv_scales[0],
        norm_gain, freq,
    )

    def run_prefill():
        return pl.pallas_call(
            functools.partial(prefill_kernel, page),
            out_shape=half_block,
            in_specs=[in_smem] + [in_vmem] * 2,
            out_specs=in_vmem,
            name="prefill",
        )(prompt_pages, query, fresh)

    def run_decode():
        span = block_tables.shape[1]
        starts = jnp.cumsum(prompt_pages) - prompt_pages
        lengths = jnp.concatenate([prompt_pages * page, cache_lens])
        own = pool.shape[0] + jnp.minimum(
            starts[:, None] + jnp.arange(span, dtype=jnp.int32)[None, :],
            page_slots.shape[0] - 1,
        )
        table = jnp.concatenate([own, block_tables], axis=0).reshape(-1)
        return pl.pallas_call(
            decode_kernel,
            out_shape=half_block,
            in_specs=[in_smem] + [in_vmem] * 4 + [in_hbm],
            out_specs=in_vmem,
            scratch_shapes=decode_scratch(
                rows, width, span * page, pool.shape[0] + rows // page, page
            ),
            compiler_params=pltpu.CompilerParams(vmem_limit_bytes=24 << 20),
            name="decode",
        )(table, lengths[:, None], query, fresh, arrived, pool)

    attended = lax.cond(side == 0, run_prefill, run_decode)

    out = pl.pallas_call(
        functools.partial(project_scatter, n),
        out_shape=half_block,
        in_specs=[in_vmem] * 3,
        out_specs=in_vmem,
        scratch_shapes=[
            VMEM((rows, width), bf16),
            VMEM((2, width, width), bf16),
            VMEM((2, 2, rows, width), f32),
            VMEM((rows, width), bf16),
            VMEM((n, rows, width), bf16),
            scatter_sems, scatter_sems, dma,
        ],
        compiler_params=pltpu.CompilerParams(
            collective_id=1, has_side_effects=True, vmem_limit_bytes=40 << 20
        ),
        cost_estimate=pl.CostEstimate(
            flops=2 * n * rows * width * width, bytes_accessed=4 << 20, transcendentals=0
        ),
        name="project_scatter",
    )(attended, o_words, o_scales)
    return out[None]


def solution(mesh):
    return jax.shard_map(
        local,
        mesh=mesh,
        in_specs=(
            P("role", "groups", "tp"),
            P(),
            P(None, "tp"),
            P(None, "tp"),
            P("tp", None, None),
            P("tp", None, None),
            P("tp", None),
            P("tp", None),
            P("tp", "groups", None, None),
            P("groups"),
            P("groups"),
            P("groups", None),
            P("groups"),
        ),
        out_specs=P("role", "groups", "tp"),
        check_vma=False,
    )
```

```python
import functools

import jax
import jax.numpy as jnp
import numpy as np
from jax import lax
from jax.experimental import pallas as pl
from jax.experimental.pallas import tpu as pltpu
from jax.sharding import PartitionSpec as P

HD = 128
LONGEST = 128
GATHER_PIECES = 4
SCATTER_PIECES = 4
REACH = 4
LEAD = 4
GATHER_VMEM = 58 << 20
MESH = pl.DeviceIdType.MESH
VMEM = pltpu.VMEM


def nibble_order(width):
    words = width // 8
    source = lax.broadcasted_iota(jnp.int32, (width, width), 0)
    column = lax.broadcasted_iota(jnp.int32, (width, width), 1)
    wanted = lax.rem(column, words) * 8 + column // words
    return jnp.where(source == wanted, 1.0, 0.0).astype(jnp.bfloat16)


def unpack_into(target, lane, words, low_scale, high_scale):
    count, width = words.shape
    half = count // 2
    scale = jnp.concatenate(
        [
            jnp.broadcast_to(low_scale, (half, width)),
            jnp.broadcast_to(high_scale, (half, width)),
        ],
        axis=0,
    )
    for k in range(8):
        nibble = jnp.bitwise_and(jnp.right_shift(words, 4 * k), 15) - 8
        value = (nibble.astype(jnp.float32) * scale).astype(jnp.bfloat16)
        target[k * count : (k + 1) * count, lane : lane + width] = value


def ring(n):
    me = lax.axis_index("tp")
    return me, lax.rem(me + 1, n), lax.rem(me + n - 1, n)


def signal_ready(peers):
    barrier = pltpu.get_barrier_semaphore()
    for peer in peers:
        pl.semaphore_signal(barrier, inc=1, device_id=peer, device_id_type=MESH)
    return barrier


def prompt_start(pages_ref, page, row):
    start, begin = jnp.zeros_like(row), 0
    for p in range(pages_ref.shape[0]):
        end = begin + pages_ref[p] * page
        start = jnp.where((row >= begin) & (row < end), begin, start)
        begin = end
    return start


def gather_project(
    page, n, pages_ref, length_ref, x_hbm, q_words, kv_words, q_scales, kv_scales, gain_ref,
    freq_ref, q_out, kv_out, fresh_out,
    x_ref, xbuf, stat, acc, weights, inverse, gains, scales, qw, kw, arrived, cosine, sine, held,
    load_sem, recv_right, recv_left, stat_right, stat_left, send_sem, stat_send, pair_sem, lead_sem,
):
    me, right, left = ring(n)
    role = lax.axis_index("role")
    half, turn = n // 2, n // 4
    rows, width = x_ref.shape
    pieces = recv_right.shape[1]
    sub = rows // pieces

    reach = min(REACH, half)
    groups = half // reach

    def behind(s):
        return lax.rem(me + n - s, n)

    def ahead(s):
        return lax.rem(me + s, n)

    peers = [{"tp": side(d)} for d in range(1, reach + 1) for side in (ahead, behind)]
    barrier = signal_ready(peers + [{"role": 1 - role}])
    load_x = pltpu.make_async_copy(x_hbm, x_ref, load_sem.at[0])
    loads = (
        pltpu.make_async_copy(q_words, qw, load_sem.at[1]),
        pltpu.make_async_copy(kv_words, kw, load_sem.at[2]),
    )
    load_x.start()
    for load in loads:
        load.start()

    order = nibble_order(width)
    load_x.wait()
    x = x_ref[...]
    xbuf[me] = jnp.dot(x, order, preferred_element_type=jnp.float32).astype(jnp.bfloat16)
    wide = x.astype(jnp.float32)
    squares = wide * wide
    folded = squares[:, 0:128]
    for lane in range(128, width, 128):
        folded = folded + squares[:, lane : lane + 128]
    stat[me] = jnp.sum(folded.T, axis=0, keepdims=True)

    def data(chunk, hop, u, to_right):
        piece = xbuf.at[chunk, pl.ds(u * sub, sub), :]
        return pltpu.make_async_remote_copy(
            src_ref=piece,
            dst_ref=piece,
            send_sem=send_sem,
            recv_sem=(recv_right if to_right else recv_left).at[hop, u],
            device_id={"tp": right if to_right else left},
            device_id_type=MESH,
        )

    def figure(chunk, sem, peer):
        return pltpu.make_async_remote_copy(
            src_ref=stat.at[chunk],
            dst_ref=stat.at[chunk],
            send_sem=stat_send,
            recv_sem=sem,
            device_id={"tp": peer},
            device_id_type=MESH,
        )

    def take_figures(g):
        for d in range(1, reach + 1):
            k = reach * (g - 1) + d
            figure(behind(k), stat_right.at[k - 1], right).wait_recv()

            @pl.when(k < half)
            def _():
                figure(ahead(k), stat_left.at[k - 1], left).wait_recv()

    def hand_on_figures(g):
        for d in range(1, reach + 1):
            k = reach * (g - 1) + d
            figure(behind(k), stat_right.at[k + reach - 1], ahead(reach)).start()

            @pl.when(k + reach < half)
            def _():
                figure(ahead(k), stat_left.at[k + reach - 1], behind(reach)).start()

    def pass_data(s, u):
        data(behind(s), s - 1, u, True).wait_recv()
        data(behind(s), s, u, True).start()
        data(ahead(s), s - 1, u, False).wait_recv()
        data(ahead(s), s, u, False).start()

    def project(chunk):
        low = scales[pl.ds(2 * chunk, 1), :]
        high = scales[pl.ds(2 * chunk + 1, 1), :]
        first = pl.multiple_of(chunk * (width // 8), width // 8)
        for lane, words in ((0, qw), (width, kw)):
            unpack_into(
                weights, lane, words[pl.ds(first, width // 8), :],
                low[:, lane : lane + width], high[:, lane : lane + width],
            )
        gain = gains[pl.ds(chunk, 1), :]
        for u in range(4):
            part = pl.ds(u * (rows // 4), rows // 4)
            scale = inverse[part, :]
            scale = jnp.concatenate([scale] * (width // 128), axis=1)
            normed = (xbuf[chunk, part, :].astype(jnp.float32) * scale * gain).astype(jnp.bfloat16)
            acc[part, :] += jnp.dot(normed, weights[...], preferred_element_type=jnp.float32)

    pl.semaphore_wait(barrier, 2 * reach + 1)

    @pl.when(role == 1)
    def _():
        pl.semaphore_wait(lead_sem, 1)

    for d in range(1, reach + 1):
        figure(me, stat_right.at[d - 1], ahead(d)).start()
        if d < half:
            figure(me, stat_left.at[d - 1], behind(d)).start()
    for u in range(pieces):
        data(me, 0, u, True).start()
        data(me, 0, u, False).start()
    for i in range(n):
        gains[i : i + 1, :] = gain_ref[i * width : (i + 1) * width].astype(jnp.float32)[None, :]
    gains[...] = jnp.dot(
        gains[...].astype(jnp.bfloat16), order, preferred_element_type=jnp.float32
    )
    scales[:, 0:width] = q_scales[...].astype(jnp.float32)
    scales[:, width:] = kv_scales[...].astype(jnp.float32)
    acc[...] = jnp.zeros_like(acc)
    row = lax.broadcasted_iota(jnp.int32, (rows, HD), 0)
    placed = (row - prompt_start(pages_ref, page, row)).astype(jnp.float32)
    prompts = pages_ref.shape[0]
    line = lax.broadcasted_iota(jnp.int32, (8, HD), 0)

    @pl.loop(0, rows // 8)
    def _(b):
        block = jnp.zeros((8, HD), jnp.int32)
        for t in range(8):
            i = 8 * b + t
            whole = pages_ref[jnp.minimum(i, prompts - 1)] * page
            length = jnp.where(i < prompts, whole, length_ref[jnp.maximum(i - prompts, 0)])
            block = jnp.where(line == t, length, block)
        held[pl.ds(pl.multiple_of(8 * b, 8), 8), :] = block.astype(jnp.float32)

    angle = jnp.where(role == 0, placed, held[...]) * freq_ref[...]
    cosine[...] = jnp.cos(angle)
    turned = jnp.sin(angle)
    lane = lax.broadcasted_iota(jnp.int32, (rows, HD), 1)
    sine[...] = jnp.where(lane < HD // 2, -turned, turned)
    for load in loads:
        load.wait()

    quarter = pieces // 4

    @pl.loop(1, turn)
    def _(s):
        @pl.when((role == 0) & (s == min(LEAD, turn - 1)))
        def _():
            pl.semaphore_signal(
                lead_sem, inc=1, device_id={"role": 1 - role}, device_id_type=MESH
            )

        for u in range(pieces):
            pass_data(s, u)
        group = (s + 1) // 2

        @pl.when((lax.rem(s, 2) == 1) & (group < groups))
        def _():
            take_figures(group)
            hand_on_figures(group)

    take_figures(groups)
    total = stat[0]
    for i in range(1, n):
        total = total + stat[i]
    mean = total / (n * width)
    inverse[...] = jnp.broadcast_to(lax.rsqrt(mean + 1e-05), (128, rows)).T

    @pl.loop(turn, half - 1)
    def _(s):
        for i in range(4):
            for u in range(i * quarter, (i + 1) * quarter):
                pass_data(s, u)
            o = 4 * (s - turn) + i
            project(behind((o + 1) // 2) if i % 2 else ahead(o // 2))

    last = half - 1
    for u in range(pieces):
        data(behind(last), last - 1, u, True).wait_recv()
        if u < pieces // 2:
            data(behind(last), last, u, True).start()
        data(ahead(last), last - 1, u, False).wait_recv()
        if u >= pieces // 2:
            data(ahead(last), last, u, False).start()
    project(ahead(last - 1))
    project(behind(last))
    project(ahead(last))
    for u in range(pieces):
        data(behind(half), last, u, u < pieces // 2).wait_recv()
    project(behind(half))

    def rotated(lane):
        head = acc[:, lane : lane + HD]
        turned = pltpu.roll(head, HD // 2, 1)
        return (head * cosine[...] + turned * sine[...]).astype(jnp.bfloat16)

    kv_out[:, 0:HD] = rotated(width)
    kv_out[:, HD:] = acc[:, width + HD :].astype(jnp.bfloat16)
    for lane in range(0, width, HD):
        q_out[:, lane : lane + HD] = rotated(lane)
    swap = pltpu.make_async_remote_copy(
        src_ref=kv_out, dst_ref=arrived, send_sem=pair_sem.at[0], recv_sem=pair_sem.at[1],
        device_id={"role": 1 - role}, device_id_type=MESH,
    )

    @pl.when(role == 0)
    def _():
        swap.start()
        fresh_out[...] = kv_out[...]
        swap.wait_send()

    @pl.when(role == 1)
    def _():
        swap.wait_recv()
        fresh_out[...] = arrived[...]

    every = xbuf.at[pl.ds(0, n - 1)]
    pltpu.make_async_copy(every, every, send_sem).wait()
    every = stat.at[pl.ds(0, n - 1)]
    pltpu.make_async_copy(every, every, stat_send).wait()


def project_scatter(
    n, att_ref, ow, scale_ref, out_ref,
    attended, weights, part, begun, slots, recv_right, recv_left, send_sem,
):
    me, right, left = ring(n)
    half = n // 2
    rows, width = att_ref.shape
    pieces = recv_right.shape[1]
    sub = rows // pieces
    barrier = signal_ready(({"tp": right}, {"tp": left}))
    attended[...] = jnp.dot(
        att_ref[...], nibble_order(width), preferred_element_type=jnp.float32
    ).astype(jnp.bfloat16)

    def unpack(side, dest):
        columns = pl.ds(pl.multiple_of(dest * width, width), width)
        scale = scale_ref[:, columns].astype(jnp.float32)
        unpack_into(weights.at[side], 0, ow[:, columns], scale[0:1, :], scale[1:2, :])

    def multiply(side, turn, i):
        block = pl.ds(i * (rows // 2), rows // 2)
        part[turn, side, block, :] = jnp.dot(
            attended[block, :], weights[side], preferred_element_type=jnp.float32
        )

    def dest(side, s):
        return lax.rem(me + half + (s if side else n - s), n)

    def token(source, side, hop, u):
        piece = pl.ds(u * sub, sub)
        return pltpu.make_async_remote_copy(
            src_ref=source.at[piece, :],
            dst_ref=slots.at[side * half + hop, piece, :],
            send_sem=send_sem,
            recv_sem=(recv_left if side else recv_right).at[hop, u],
            device_id={"tp": left if side else right},
            device_id_type=MESH,
        )

    def slot(side, hop):
        return slots.at[side * half + hop]

    unpack(0, dest(0, 0))
    for i in range(2):
        multiply(0, 0, i)
    begun[...] = part[0, 0].astype(jnp.bfloat16)
    pl.semaphore_wait(barrier, 2)
    for u in range(pieces):
        token(begun, 2 * u // pieces, 0, u).start()
    for side in range(2):
        unpack(side, dest(side, 1))
        for i in range(2):
            multiply(side, 1, i)

    def ahead(s, turn, task):
        side = task % 2
        if task < 2:
            unpack(side, dest(side, s))
        else:
            multiply(side, turn, (task - 2) // 2)

    def step(s, joins):
        now, later = lax.rem(s, 2), lax.rem(s + 1, 2)
        for u in range(pieces):
            piece = pl.ds(u * sub, sub)
            for side in range(2):
                here = slot(side, s - 1)
                term = part[now, side, piece, :]
                if joins(side, u):
                    token(here, side, s - 1, u).wait_recv()
                    term = term + here[piece, :].astype(jnp.float32)
                here[piece, :] = term.astype(jnp.bfloat16)
                token(here, side, s, u).start()
            for task in range(6 * u // pieces, 6 * (u + 1) // pieces):
                ahead(s + 1, later, task)

    step(1, lambda side, u: side == 2 * u // pieces)

    @pl.loop(2, half)
    def _(s):
        step(s, lambda side, u: True)

    for u in range(pieces):
        piece = pl.ds(u * sub, sub)
        term = part[half % 2, 0, piece, :]
        for side in range(2):
            here = slot(side, half - 1)
            token(here, side, half - 1, u).wait_recv()
            term = term + here[piece, :].astype(jnp.float32)
        out_ref[piece, :] = term.astype(jnp.bfloat16)
    every = slots.at[pl.ds(0, n - 1)]
    pltpu.make_async_copy(every, every, send_sem).wait()


def prefill_kernel(page, pages_ref, q_ref, kv_ref, out_ref):
    rows = q_ref.shape[0]
    block = min(LONGEST, rows)
    for first in range(0, rows, block):
        low = max(0, first - LONGEST)
        count = first + block - low
        keys = kv_ref[low : first + block, 0:HD]
        values = kv_ref[low : first + block, HD:]
        row = lax.broadcasted_iota(jnp.int32, (block, count), 0) + first
        key = lax.broadcasted_iota(jnp.int32, (block, count), 1) + low
        start = prompt_start(pages_ref, page, row)
        allowed = (key <= row) & (key >= start)
        for lane in range(0, q_ref.shape[1], HD):
            query = q_ref[first : first + block, lane : lane + HD]
            scores = lax.dot_general(
                query, keys, (((1,), (1,)), ((), ())), preferred_element_type=jnp.float32
            ) * (HD**-0.5)
            scores = jnp.where(allowed, scores, -1e30)
            top = jnp.max(scores, axis=1, keepdims=True)
            raised = jnp.exp(scores - top)
            weight = raised * (1.0 / jnp.sum(raised, axis=1, keepdims=True))
            out_ref[first : first + block, lane : lane + HD] = jnp.dot(
                weight.astype(jnp.bfloat16), values, preferred_element_type=jnp.float32
            ).astype(jnp.bfloat16)


def decode_scratch(rows, width, tokens, pages, page):
    return [
        VMEM((pages, page, 2 * HD), jnp.bfloat16),
        VMEM((rows, width), jnp.float32),
        VMEM((rows, 2 * HD), jnp.float32),
        VMEM((2 * rows, tokens), jnp.float32),
        VMEM((2 * rows, HD), jnp.float32),
        VMEM((2 * rows, tokens), jnp.bfloat16),
        VMEM((rows, width), jnp.float32),
        pltpu.SemaphoreType.DMA,
    ]


def decode_kernel(
    table_ref, length_ref, q_ref, kv_ref, fresh_ref, pool_ref, out_ref,
    cache, q_wide, kv_wide, score_buf, self_buf, weight_buf, out_wide, load_sem,
):
    rows = q_ref.shape[0]
    pool, page, _ = pool_ref.shape
    span = table_ref.shape[0] // rows
    load = pltpu.make_async_copy(pool_ref, cache.at[pl.ds(0, pool)], load_sem)
    load.start()
    for j in range(rows // page):
        cache[pool + j] = fresh_ref[j * page : (j + 1) * page, :]
    q_wide[...] = q_ref[...].astype(jnp.float32)
    kv_wide[...] = kv_ref[...].astype(jnp.float32)
    load.wait()
    batch = 8
    owner = lax.rem(lax.broadcasted_iota(jnp.int32, (2 * batch, HD), 0), batch)
    spot = lax.broadcasted_iota(jnp.int32, (2 * batch, span * page), 1)

    def gathered(first, lane):
        pages = []
        for j in range(span):
            pair = [
                cache[table_ref[(first + t) * span + j], :, lane : lane + HD] for t in range(2)
            ]
            pages.append(jnp.concatenate(pair, axis=1))
        return jnp.concatenate(pages, axis=0)

    def twice(piece, ref, lane):
        return jnp.concatenate([ref[piece, lane : lane + HD]] * 2, axis=0)

    def score_block(b):
        first = pl.multiple_of(b * batch, batch)
        piece = pl.ds(first, batch)
        both = q_wide[piece, :]
        query = jnp.concatenate([both[:, 0:HD], both[:, HD:]], axis=0)
        length = jnp.concatenate([length_ref[piece, :]] * 2, axis=0)
        scores = None
        for p in range(0, batch, 2):
            mine = jnp.concatenate(
                [jnp.where(owner == p + t, query, 0.0) for t in range(2)], axis=1
            ).astype(jnp.bfloat16)
            term = lax.dot_general(
                mine, gathered(first + p, 0), (((1,), (1,)), ((), ())),
                preferred_element_type=jnp.float32,
            )
            scores = term if scores is None else scores + term
        out = pl.ds(2 * first, 2 * batch)
        score_buf[out, :] = jnp.where(spot < length, scores * (HD**-0.5), -1e30)
        self_score = jnp.sum(query * twice(piece, kv_wide, 0), axis=1, keepdims=True)
        self_buf[out, :] = jnp.broadcast_to(self_score * (HD**-0.5), (2 * batch, HD))

    def weigh(i):
        piece = pl.ds(i * 128, 128)
        scores, self_score = score_buf[piece, :], self_buf[piece, :]
        top = jnp.maximum(jnp.max(scores, axis=1, keepdims=True), self_score)
        raised = jnp.exp(scores - jnp.concatenate([top] * (scores.shape[1] // HD), axis=1))
        self_raised = jnp.exp(self_score - top)
        share = 1.0 / (jnp.sum(raised, axis=1, keepdims=True) + self_raised)
        share = jnp.broadcast_to(share, self_score.shape)
        weight_buf[piece, :] = (
            raised * jnp.concatenate([share] * (scores.shape[1] // HD), axis=1)
        ).astype(jnp.bfloat16)
        self_buf[piece, :] = (self_raised * share).astype(jnp.bfloat16).astype(jnp.float32)

    def value_block(b):
        first = pl.multiple_of(b * batch, batch)
        piece = pl.ds(first, batch)
        weight = weight_buf[pl.ds(2 * first, 2 * batch), :]
        total = self_buf[pl.ds(2 * first, 2 * batch), :] * twice(piece, kv_wide, HD)
        for p in range(0, batch, 2):
            term = jnp.dot(weight, gathered(first + p, HD), preferred_element_type=jnp.float32)
            for t in range(2):
                total = total + jnp.where(owner == p + t, term[:, t * HD : (t + 1) * HD], 0.0)
        out_wide[piece, 0:HD] = total[0:batch, :]
        out_wide[piece, HD:] = total[batch:, :]

    @pl.loop(0, rows // batch, step=4)
    def _(b):
        for i in range(4):
            score_block(b + i)

    @pl.loop(0, 2 * rows // 128)
    def _(i):
        weigh(i)

    @pl.loop(0, rows // batch, step=4)
    def _(b):
        for i in range(4):
            value_block(b + i)

    out_ref[...] = out_wide[...].astype(jnp.bfloat16)


def local(
    rows_in, norm_gain, q_words, q_scales, kv_words, kv_scales, o_words, o_scales,
    kv_pool, prompt_pages, page_slots, block_tables, cache_lens,
):
    n = lax.axis_size("tp")
    side = lax.axis_index("role")
    x = rows_in[0]
    rows, width = x.shape
    half = n // 2
    pool = kv_pool[0]
    page = pool.shape[1]
    count = prompt_pages.shape[0]
    dma = pltpu.SemaphoreType.DMA
    gather_sems, scatter_sems = dma((half, GATHER_PIECES)), dma((half, SCATTER_PIECES))
    in_vmem = pl.BlockSpec(memory_space=VMEM)
    in_smem = pl.BlockSpec(memory_space=pltpu.SMEM)
    in_hbm = pl.BlockSpec(memory_space=pltpu.HBM)
    bf16, f32 = jnp.bfloat16, jnp.float32

    freq = np.float32(500000.0) ** (-np.arange(HD // 2, dtype=np.float32) * 2 / HD)
    freq = jnp.asarray(np.concatenate([freq, freq])[None, :].astype(np.float32))

    half_block = jax.ShapeDtypeStruct((rows, width), bf16)
    query, fresh, arrived = pl.pallas_call(
        functools.partial(gather_project, page, n),
        out_shape=(
            half_block,
            jax.ShapeDtypeStruct((rows, 2 * HD), bf16),
            jax.ShapeDtypeStruct((rows, 2 * HD), bf16),
        ),
        in_specs=[in_smem] * 2 + [in_hbm] * 3 + [in_vmem] * 4,
        out_specs=(in_vmem, in_vmem, in_vmem),
        scratch_shapes=[
            VMEM((rows, width), bf16),
            VMEM((n, rows, width), bf16),
            VMEM((n, 1, rows), f32),
            VMEM((rows, width + 2 * HD), f32),
            VMEM((width, width + 2 * HD), bf16),
            VMEM((rows, 128), f32),
            VMEM((n, width), f32),
            VMEM((q_scales.shape[0], width + 2 * HD), f32),
            VMEM(q_words.shape, jnp.int32),
            VMEM(kv_words.shape[1:], jnp.int32),
            VMEM((rows, 2 * HD), bf16),
            VMEM((rows, HD), f32),
            VMEM((rows, HD), f32),
            VMEM((rows, HD), f32),
            dma((3,)), gather_sems, gather_sems, dma((half,)), dma((half,)),
            dma, dma, dma((2,)), pltpu.SemaphoreType.REGULAR,
        ],
        compiler_params=pltpu.CompilerParams(
            collective_id=0, has_side_effects=True, vmem_limit_bytes=GATHER_VMEM
        ),
        cost_estimate=pl.CostEstimate(
            flops=4 * n * rows * width * width, bytes_accessed=4 << 20, transcendentals=0
        ),
        name="gather_project",
    )(
        prompt_pages, cache_lens, x, q_words, kv_words[0], q_scales, kv_scales[0],
        norm_gain, freq,
    )

    def run_prefill():
        return pl.pallas_call(
            functools.partial(prefill_kernel, page),
            out_shape=half_block,
            in_specs=[in_smem] + [in_vmem] * 2,
            out_specs=in_vmem,
            name="prefill",
        )(prompt_pages, query, fresh)

    def run_decode():
        span = block_tables.shape[1]
        starts = jnp.cumsum(prompt_pages) - prompt_pages
        lengths = jnp.concatenate([prompt_pages * page, cache_lens])
        own = pool.shape[0] + jnp.minimum(
            starts[:, None] + jnp.arange(span, dtype=jnp.int32)[None, :],
            page_slots.shape[0] - 1,
        )
        table = jnp.concatenate([own, block_tables], axis=0).reshape(-1)
        return pl.pallas_call(
            decode_kernel,
            out_shape=half_block,
            in_specs=[in_smem] + [in_vmem] * 4 + [in_hbm],
            out_specs=in_vmem,
            scratch_shapes=decode_scratch(
                rows, width, span * page, pool.shape[0] + rows // page, page
            ),
            compiler_params=pltpu.CompilerParams(vmem_limit_bytes=24 << 20),
            name="decode",
        )(table, lengths[:, None], query, fresh, arrived, pool)

    attended = lax.cond(side == 0, run_prefill, run_decode)

    out = pl.pallas_call(
        functools.partial(project_scatter, n),
        out_shape=half_block,
        in_specs=[in_vmem] * 3,
        out_specs=in_vmem,
        scratch_shapes=[
            VMEM((rows, width), bf16),
            VMEM((2, width, width), bf16),
            VMEM((2, 2, rows, width), f32),
            VMEM((rows, width), bf16),
            VMEM((n, rows, width), bf16),
            scatter_sems, scatter_sems, dma,
        ],
        compiler_params=pltpu.CompilerParams(
            collective_id=1, has_side_effects=True, vmem_limit_bytes=40 << 20
        ),
        cost_estimate=pl.CostEstimate(
            flops=2 * n * rows * width * width, bytes_accessed=4 << 20, transcendentals=0
        ),
        name="project_scatter",
    )(attended, o_words, o_scales)
    return out[None]


def solution(mesh):
    return jax.shard_map(
        local,
        mesh=mesh,
        in_specs=(
            P("role", "groups", "tp"),
            P(),
            P(None, "tp"),
            P(None, "tp"),
            P("tp", None, None),
            P("tp", None, None),
            P("tp", None),
            P("tp", None),
            P("tp", "groups", None, None),
            P("groups"),
            P("groups"),
            P("groups", None),
            P("groups"),
        ),
        out_specs=P("role", "groups", "tp"),
        check_vma=False,
    )
```
